16 devices in a mesh: fsdp: 16 (over z, y, x, core).
Axes of the slice: x: 2, y: 2, z: 2, core: 2. Of those that a mesh axis runs over, the one named last changes fastest.
Arguments:
- x_layers: bfloat16 [2, 16, 2048, 768], P(None, 'fsdp')
- dy_top: bfloat16 [16, 2048, 768], P('fsdp')
- x_next: bfloat16 [16, 2048, 768], P('fsdp')
- w_up: bfloat16 [2, 768, 3072], replicated
- w_down: bfloat16 [2, 3072, 768], replicated
- acc_up: float32 [2, 768, 3072], P(None, 'fsdp')
- acc_down: float32 [2, 3072, 768], P(None, 'fsdp')
- master_up: float32 [2, 768, 3072], P(None, 'fsdp')
- master_down: float32 [2, 3072, 768], P(None, 'fsdp')
- mom_up: float32 [2, 768, 3072], P(None, 'fsdp')
- mom_down: float32 [2, 3072, 768], P(None, 'fsdp')
- var_up: float32 [2, 768, 3072], P(None, 'fsdp')
- var_down: float32 [2, 3072, 768], P(None, 'fsdp')
Outputs:
- output 1: float32 [2, 768, 3072], P(None, 'fsdp')
- output 2: float32 [2, 3072, 768], P(None, 'fsdp')
- output 3: float32 [2, 768, 3072], P(None, 'fsdp')
- output 4: float32 [2, 3072, 768], P(None, 'fsdp')
- output 5: float32 [2, 768, 3072], P(None, 'fsdp')
- output 6: float32 [2, 3072, 768], P(None, 'fsdp')
- output 7: bfloat16 [16, 2048, 768], P('fsdp')
All inputs are finite; a program needn't handle non-finite values.
Results may differ from the reference program's by a relative error of at most 0.00956.
Values are sent between devices in bfloat16 or wider.
A program may use at most 1 GiB of HBM per device.

```python
import jax
import jax.numpy as jnp
from jax import lax

D = 768
FF = 3072
LAYERS = 2
GROUP_SIZE = 16
BATCH_DEV = 1
SEQ_LEN = 2048
MICRO_STEPS = 2
STEP_COUNT = 3

BETA_MOM = 0.9
BETA_VAR = 0.999
ADAM_EPS = 1e-6
WEIGHT_DECAY = 0.01
LEARN_RATE = 0.06

BATCH = GROUP_SIZE * BATCH_DEV


def row_profile(rng_key, row_count):
    increments = jax.random.normal(rng_key, (LAYERS, row_count, 1), jnp.float32)
    log_scale = jnp.cumsum(increments, axis=1) * row_count ** -0.5
    scales = jnp.exp(log_scale)
    return scales / jnp.sqrt(jnp.mean(scales * scales, axis=1, keepdims=True))


def setup_inputs(seed: int = 0) -> dict:
    key_list = jax.random.split(jax.random.key(seed), 16)
    tok_count = BATCH * SEQ_LEN
    tok_shape = (BATCH, SEQ_LEN, D)
    up_shape = (LAYERS, D, FF)
    down_shape = (LAYERS, FF, D)
    x_layers = jax.random.normal(key_list[0], (LAYERS,) + tok_shape, jnp.float32)
    dy_top = jax.random.normal(key_list[1], tok_shape, jnp.float32) * tok_count ** -0.5
    x_next = jax.random.normal(key_list[2], tok_shape, jnp.float32)
    master_up = jax.random.normal(key_list[3], up_shape, jnp.float32) * row_profile(key_list[4], D) * D ** -0.5
    master_down = jax.random.normal(key_list[5], down_shape, jnp.float32) * row_profile(key_list[6], FF) * FF ** -0.5
    acc_up = 0.6 * jax.random.normal(key_list[7], up_shape, jnp.float32)
    acc_down = 0.6 * jax.random.normal(key_list[8], down_shape, jnp.float32)
    mom_up = 0.08 * jax.random.normal(key_list[9], up_shape, jnp.float32)
    mom_down = 0.08 * jax.random.normal(key_list[10], down_shape, jnp.float32)
    sq_up = jnp.sum(jnp.square(jax.random.normal(key_list[11], (2,) + up_shape, jnp.float32)), axis=0)
    sq_down = jnp.sum(jnp.square(jax.random.normal(key_list[12], (2,) + down_shape, jnp.float32)), axis=0)
    var_up = 0.0003 * (0.5 + sq_up)
    var_down = 0.0003 * (0.5 + sq_down)
    return {
        'x_layers': x_layers.astype(jnp.bfloat16),
        'dy_top': dy_top.astype(jnp.bfloat16),
        'x_next': x_next.astype(jnp.bfloat16),
        'w_up': master_up.astype(jnp.bfloat16),
        'w_down': master_down.astype(jnp.bfloat16),
        'acc_up': acc_up,
        'acc_down': acc_down,
        'master_up': master_up,
        'master_down': master_down,
        'mom_up': mom_up,
        'mom_down': mom_down,
        'var_up': var_up,
        'var_down': var_down,
    }


def lamb_step(grad_sum, acc_prev, master, mom_prev, var_prev):
    grad_full = (acc_prev + grad_sum) / MICRO_STEPS
    mom_new = BETA_MOM * mom_prev + (1.0 - BETA_MOM) * grad_full
    var_new = BETA_VAR * var_prev + (1.0 - BETA_VAR) * grad_full * grad_full
    update = (mom_new / (1.0 - BETA_MOM ** STEP_COUNT)) / (jnp.sqrt(var_new / (1.0 - BETA_VAR ** STEP_COUNT)) + ADAM_EPS) + WEIGHT_DECAY * master
    w_norm = jnp.sqrt(jnp.sum(master * master, axis=(1, 2), keepdims=True))
    u_norm = jnp.sqrt(jnp.sum(update * update, axis=(1, 2), keepdims=True))
    return master - LEARN_RATE * (w_norm / u_norm) * update, mom_new, var_new


def reference(x_layers, dy_top, x_next, w_up, w_down, acc_up, acc_down, master_up, master_down, mom_up, mom_down, var_up, var_down):
    x_dev = jnp.moveaxis(x_layers, 0, 1).reshape(GROUP_SIZE, BATCH_DEV, LAYERS, SEQ_LEN, D)
    dy_dev = dy_top.reshape(GROUP_SIZE, BATCH_DEV, SEQ_LEN, D)
    zero_init = (jnp.zeros((LAYERS, D, FF), jnp.float32), jnp.zeros((LAYERS, FF, D), jnp.float32))

    def seq_grads(carry_sum, seq_item):
        x_seq, d_cur = seq_item
        grads_up = [None] * LAYERS
        grads_down = [None] * LAYERS
        for layer_id in reversed(range(LAYERS)):
            x_cur = x_seq[layer_id]
            pre_act = jnp.dot(x_cur, w_up[layer_id], preferred_element_type=jnp.float32)
            act_f32, gelu_vjp = jax.vjp(jax.nn.gelu, pre_act)
            act_bf = act_f32.astype(jnp.bfloat16)
            d_act = jnp.dot(d_cur, w_down[layer_id].T, preferred_element_type=jnp.float32)
            d_pre = gelu_vjp(d_act)[0].astype(jnp.bfloat16)
            grads_down[layer_id] = jnp.dot(act_bf.T, d_cur, preferred_element_type=jnp.float32)
            grads_up[layer_id] = jnp.dot(x_cur.T, d_pre, preferred_element_type=jnp.float32)
            if layer_id > 0:
                d_cur = (d_cur.astype(jnp.float32) + jnp.dot(d_pre, w_up[layer_id].T, preferred_element_type=jnp.float32)).astype(jnp.bfloat16)
        return (carry_sum[0] + jnp.stack(grads_up), carry_sum[1] + jnp.stack(grads_down)), None

    def device_grads(carry_sum, dev_item):
        part_sum, _ = lax.scan(seq_grads, zero_init, dev_item)
        return (carry_sum[0] + part_sum[0].astype(jnp.bfloat16).astype(jnp.float32), carry_sum[1] + part_sum[1].astype(jnp.bfloat16).astype(jnp.float32)), None

    grad_total, _ = lax.scan(device_grads, zero_init, (x_dev, dy_dev))
    up_new, up_mom, up_var = lamb_step(grad_total[0], acc_up, master_up, mom_up, var_up)
    down_new, down_mom, down_var = lamb_step(grad_total[1], acc_down, master_down, mom_down, var_down)
    w_up_new = up_new.astype(jnp.bfloat16)
    w_down_new = down_new.astype(jnp.bfloat16)

    def forward_seq(x_seq):
        for layer_id in range(LAYERS):
            pre_act = jnp.dot(x_seq, w_up_new[layer_id], preferred_element_type=jnp.float32)
            act_bf = jax.nn.gelu(pre_act).astype(jnp.bfloat16)
            mlp_out = jnp.dot(act_bf, w_down_new[layer_id], preferred_element_type=jnp.float32)
            x_seq = (x_seq.astype(jnp.float32) + mlp_out).astype(jnp.bfloat16)
        return x_seq

    x_out = lax.map(forward_seq, x_next)
    return (up_new, down_new, up_mom, down_mom, up_var, down_var, x_out)
```

```python
import functools

import jax
import jax.numpy as jnp
from jax import lax
from jax.experimental import pallas as pl
from jax.experimental.pallas import tpu as pltpu
from jax.sharding import PartitionSpec as P

MICRO_STEPS = 2
STEP_COUNT = 3
BETA_MOM = 0.9
BETA_VAR = 0.999
ADAM_EPS = 1e-6
WEIGHT_DECAY = 0.01
LEARN_RATE = 0.06
NDEV = 16
MESH = pl.DeviceIdType.MESH
F32 = jnp.float32
BF16 = jnp.bfloat16

KINDS = {'up': (48, 3072, 512), 'dn': (192, 768, 768)}
ORDER = (('up', 0), ('dn', 0), ('up', 1), ('dn', 1))
DIM_ORDERS = ((0, 1, 2), (1, 2, 0), (2, 0, 1))


def gelu_tanh(v):
    return v * (0.5 * (1.0 + jnp.tanh(0.7978845608028654 * (v + 0.044715 * (v * v * v)))))


def step_kernel(*refs):
    (p_up0, p_dn0, p_up1, p_dn1, acc_up, acc_dn, mas_up, mas_dn, mom_up, mom_dn, var_up, var_dn, x_hbm,
     o_mas_up, o_mas_dn, o_mom_up, o_mom_dn, o_var_up, o_var_dn, o_x,
     wu, wd, r0u, r0d, q1u, q1d, q2u, q2d, q3u, q3d, stu, std, xa, xb, act, norms,
     ld_sem, out_sem, rs_send, rs_recv, ag_send, ag_recv, dd_send, dd_recv, nm_send, nm_recv) = refs
    parts_hbm = {('up', 0): p_up0, ('dn', 0): p_dn0, ('up', 1): p_up1, ('dn', 1): p_dn1}
    whole = {'up': wu, 'dn': wd}
    recv0 = {'up': r0u, 'dn': r0d}
    recvs = {'up': (q1u, q2u, q3u), 'dn': (q1d, q2d, q3d)}
    state = {'up': stu, 'dn': std}
    state_in = {'up': (acc_up, mas_up, mom_up, var_up), 'dn': (acc_dn, mas_dn, mom_dn, var_dn)}
    state_out = {'up': (o_mas_up, o_mom_up, o_var_up), 'dn': (o_mas_dn, o_mom_dn, o_var_dn)}

    me = lax.axis_index('fsdp')
    bits = (me // 8, (me // 4) % 2, (me // 2) % 2)
    core = me % 2
    partner = me + 1 - 2 * core
    neighbours = tuple(me + step * (1 - 2 * bit) for bit, step in zip(bits, (8, 4, 2)))

    loads = []
    for m, (kind, layer) in enumerate(ORDER):
        loads.append(pltpu.make_async_copy(parts_hbm[(kind, layer)], whole[kind].at[layer], ld_sem.at[m]))
    for m, (kind, layer) in enumerate(ORDER):
        for k in range(4):
            loads.append(pltpu.make_async_copy(state_in[kind][k].at[layer], state[kind].at[layer, k], ld_sem.at[4 + 4 * m + k]))
    loads.append(pltpu.make_async_copy(x_hbm.at[0], xa, ld_sem.at[20]))
    for copy in loads:
        copy.start()

    barrier = pltpu.get_barrier_semaphore()

    def hello(k, carry):
        pl.semaphore_signal(barrier, inc=1, device_id=(lax.rem(me + k, NDEV),), device_id_type=MESH)
        return carry

    lax.fori_loop(1, NDEV, hello, 0)
    pl.semaphore_wait(barrier, NDEV - 1)

    def remote(src, dst, send, recv, device):
        return pltpu.make_async_remote_copy(src_ref=src, dst_ref=dst, send_sem=send, recv_sem=recv, device_id=(device,), device_id_type=MESH)

    def place(fixed):
        return tuple(fixed.get(d, slice(None)) for d in range(3))

    flights = {}
    out_copies = []

    def rs0_start(m):
        kind, layer = ORDER[m]
        loads[m].wait()
        flights[m, 'rs0'] = remote(whole[kind].at[layer, :, :, :, 1 - core], recv0[kind].at[layer], rs_send.at[m, 0], rs_recv.at[m, 0], partner)
        flights[m, 'rs0'].start()

    def rs_start(m, stage):
        kind, layer = ORDER[m]
        third = KINDS[kind][0] // 3
        for p, dims in enumerate(DIM_ORDERS):
            fixed = {d: bits[d] for d in dims[:stage]}
            fixed[dims[stage]] = 1 - bits[dims[stage]]
            src = recv0[kind].at[(layer,) + place(fixed) + (pl.ds(third * p, third),)]
            flights[m, 'rs', stage, p] = remote(src, recvs[kind][stage].at[layer, p], rs_send.at[m, 1 + 3 * stage + p], rs_recv.at[m, 1 + 3 * stage + p], neighbours[dims[stage]])
            flights[m, 'rs', stage, p].start()

    def rs0_finish(m):
        kind, layer = ORDER[m]
        flights[m, 'rs0'].wait()
        buf, mine = recv0[kind], whole[kind]

        def add(i, carry):
            z, y, x = i // 4, (i // 2) % 2, i % 2
            buf[layer, z, y, x] = buf[layer, z, y, x] + mine[layer, z, y, x, core]
            return carry

        lax.fori_loop(0, 8, add, 0)
        rs_start(m, 0)

    def rs_finish(m, stage):
        kind, layer = ORDER[m]
        third = KINDS[kind][0] // 3
        buf, got = recv0[kind], recvs[kind][stage]
        for p, dims in enumerate(DIM_ORDERS):
            flights[m, 'rs', stage, p].wait()
            rest = dims[stage + 1:]
            free = [d for d in range(3) if d in rest]
            for i in range(2 ** len(free)):
                where = {d: bits[d] for d in dims[:stage + 1]}
                slot = []
                for j, d in enumerate(free):
                    where[d] = (i >> (len(free) - 1 - j)) & 1
                    slot.append(where[d])
                idx = (layer,) + place(where) + (pl.ds(third * p, third),)
                buf[idx] = buf[idx] + got[(layer, p) + tuple(slot)]
        rs_start(m, stage + 1)

    def lamb(m):
        kind, layer = ORDER[m]
        rows, cols, wide = KINDS[kind]
        third = rows // 3
        buf, got, st = recv0[kind], recvs[kind][2], state[kind]
        for k in range(4):
            loads[4 + 4 * m + k].wait()
        per_row = cols // wide
        w_sum = jnp.zeros((16, wide), F32)
        u_sum = jnp.zeros((16, wide), F32)
        for p in range(3):
            flights[m, 'rs', 2, p].wait()

            def chunk(i, carry):
                w_acc, u_acc = carry
                row, col = i // per_row, i % per_row
                cs = pl.ds(pl.multiple_of(col * wide, wide), wide)
                local = pl.ds(pl.multiple_of(row * 16, 16), 16)
                glob = pl.ds(pl.multiple_of(third * p + row * 16, 16), 16)
                total = buf[layer, bits[0], bits[1], bits[2], glob, cs].astype(F32) + got[layer, p, local, cs].astype(F32)
                master = st[layer, 1, glob, cs]
                grad = (st[layer, 0, glob, cs] + total) / MICRO_STEPS
                mom = BETA_MOM * st[layer, 2, glob, cs] + (1.0 - BETA_MOM) * grad
                var = BETA_VAR * st[layer, 3, glob, cs] + (1.0 - BETA_VAR) * grad * grad
                upd = (mom / (1.0 - BETA_MOM ** STEP_COUNT)) / (jnp.sqrt(var / (1.0 - BETA_VAR ** STEP_COUNT)) + ADAM_EPS) + WEIGHT_DECAY * master
                st[layer, 0, glob, cs] = upd
                st[layer, 2, glob, cs] = mom
                st[layer, 3, glob, cs] = var
                return w_acc + master * master, u_acc + upd * upd

            w_sum, u_sum = lax.fori_loop(0, (third // 16) * per_row, chunk, (w_sum, u_sum))

        def fold(v):
            tiles = [v[8 * i:8 * i + 8, 128 * j:128 * j + 128] for i in range(2) for j in range(wide // 128)]
            return functools.reduce(lambda a, b: a + b, tiles)

        norms[m, me, 0:8] = fold(w_sum)
        norms[m, me, 8:16] = fold(u_sum)
        for k, o in ((2, 1), (3, 2)):
            copy = pltpu.make_async_copy(st.at[layer, k], state_out[kind][o].at[layer], out_sem.at[3 * m + o])
            copy.start()
            out_copies.append(copy)

        def tell(k, carry):
            remote(norms.at[m, me], norms.at[m, me], nm_send.at[m], nm_recv.at[m], lax.rem(me + k, NDEV)).start()
            return carry

        lax.fori_loop(1, NDEV, tell, 0)

    def apply(m):
        kind, layer = ORDER[m]
        rows, cols, wide = KINDS[kind]
        st = state[kind]
        for sem in (nm_send, nm_recv):
            pltpu.make_async_copy(norms.at[m, pl.ds(0, NDEV - 1)], norms.at[m, pl.ds(0, NDEV - 1)], sem.at[m]).wait()
        sums = jnp.sum(norms[m], axis=0)
        w_sq = jnp.sum(jnp.sum(sums[0:8], axis=0, keepdims=True), axis=1, keepdims=True)
        u_sq = jnp.sum(jnp.sum(sums[8:16], axis=0, keepdims=True), axis=1, keepdims=True)
        scale = LEARN_RATE * (jnp.sqrt(w_sq) / jnp.sqrt(u_sq))
        per_row = cols // wide

        def chunk(i, carry):
            row, col = i // per_row, i % per_row
            at = (pl.ds(pl.multiple_of(row * 16, 16), 16), pl.ds(pl.multiple_of(col * wide, wide), wide))
            new = st[(layer, 1) + at] - scale * st[(layer, 0) + at]
            st[(layer, 1) + at] = new
            whole[kind][(layer, bits[0], bits[1], bits[2], core) + at] = new.astype(BF16)
            return carry

        lax.fori_loop(0, (rows // 16) * per_row, chunk, 0)
        copy = pltpu.make_async_copy(st.at[layer, 1], state_out[kind][0].at[layer], out_sem.at[3 * m])
        copy.start()
        out_copies.append(copy)
        ag_start(m, 0)
        ref = whole[kind].at[layer, bits[0], bits[1], bits[2], core]
        flights[m, 'dd'] = remote(ref, ref, dd_send.at[m, 0], dd_recv.at[m, 0], partner)
        flights[m, 'dd'].start()

    def ag_start(m, stage):
        kind, layer = ORDER[m]
        third = KINDS[kind][0] // 3
        for p, dims in enumerate(DIM_ORDERS):
            fixed = {d: bits[d] for d in dims[:3 - stage]}
            ref = whole[kind].at[(layer,) + place(fixed) + (core, pl.ds(third * p, third))]
            flights[m, 'ag', stage, p] = remote(ref, ref, ag_send.at[m, 3 * stage + p], ag_recv.at[m, 3 * stage + p], neighbours[dims[2 - stage]])
            flights[m, 'ag', stage, p].start()

    def ag_finish(m, stage):
        kind, layer = ORDER[m]
        third = KINDS[kind][0] // 3
        for p in range(3):
            flights[m, 'ag', stage, p].wait()
        if stage < 2:
            ag_start(m, stage + 1)
        for p, dims in enumerate(DIM_ORDERS):
            fixed = {d: bits[d] for d in dims[:2 - stage]}
            fixed[dims[2 - stage]] = 1 - bits[dims[2 - stage]]
            ref = whole[kind].at[(layer,) + place(fixed) + (core, pl.ds(third * p, third))]
            flights[m, 'dd', stage, p] = remote(ref, ref, dd_send.at[m, 1 + 3 * stage + p], dd_recv.at[m, 1 + 3 * stage + p], partner)
            flights[m, 'dd', stage, p].start()

    def ag_done(m):
        flights[m, 'dd'].wait()
        for stage in range(3):
            for p in range(3):
                flights[m, 'dd', stage, p].wait()

    stages = (
        rs0_finish,
        lambda m: rs_finish(m, 0),
        lambda m: rs_finish(m, 1),
        lamb,
        apply,
        lambda m: ag_finish(m, 0),
        lambda m: ag_finish(m, 1),
        lambda m: ag_finish(m, 2),
        ag_done,
    )
    for m in range(4):
        rs0_start(m)
    tasks = [(m, t - m) for t in range(len(stages) + 3) for m in range(4) if 0 <= t - m < len(stages)]

    def run_next():
        if tasks:
            m, s = tasks.pop(0)
            stages[s](m)

    def need(m):
        while (m, len(stages) - 1) in tasks:
            run_next()

    half = act.shape[0]
    loads[20].wait()

    def up_chunk(layer, src, base, lo, hi):
        def body(n, carry):
            cs = pl.ds(pl.multiple_of(n * 512, 512), 512)
            w = wu[layer, :, :, :, :, :, cs].reshape(768, 512)

            def rows(i, carry):
                at = pl.ds(pl.multiple_of(i * 512, 512), 512)
                pre = jnp.dot(src[pl.ds(pl.multiple_of(base + i * 512, 512), 512), :], w, preferred_element_type=F32)
                act[at, cs] = gelu_tanh(pre).astype(BF16)
                return carry

            return lax.fori_loop(0, half // 512, rows, carry)

        lax.fori_loop(lo, hi, body, 0)

    def down_chunk(layer, src, dst, base):
        def body(i, carry):
            at = pl.ds(pl.multiple_of(base + i * 256, 256), 256)
            w = wd[layer].reshape(3072, 768)
            out = jnp.dot(act[pl.ds(pl.multiple_of(i * 256, 256), 256), :], w, preferred_element_type=F32)
            dst[at, :] = (src[at, :].astype(F32) + out).astype(BF16)
            return carry

        lax.fori_loop(0, half // 256, body, 0)

    for layer, src, dst in ((0, xa, xb), (1, xb, xa)):
        for base in range(0, 2048, half):
            need(2 * layer)
            up_chunk(layer, src, base, 0, 3)
            run_next()
            up_chunk(layer, src, base, 3, 6)
            need(2 * layer + 1)
            down_chunk(layer, src, dst, base)
            run_next()
            if layer == 1:
                copy = pltpu.make_async_copy(dst.at[pl.ds(base, half)], o_x.at[0, pl.ds(base, half)], out_sem.at[12 + base // half])
                copy.start()
                out_copies.append(copy)
    for copy in out_copies:
        copy.wait()


def gather_step(parts, states, x_next):
    def blocks(rows, cols):
        return (2, 2, 2, 2, 2, rows, cols)

    scratch = [pltpu.VMEM(blocks(r, c), BF16) for r, c, _ in KINDS.values()]
    scratch += [pltpu.VMEM((2, 2, 2, 2, r, c), BF16) for r, c, _ in KINDS.values()]
    scratch += [pltpu.VMEM((2, 3, 2, 2, r // 3, c), BF16) for r, c, _ in KINDS.values()]
    scratch += [pltpu.VMEM((2, 3, 2, r // 3, c), BF16) for r, c, _ in KINDS.values()]
    scratch += [pltpu.VMEM((2, 3, r // 3, c), BF16) for r, c, _ in KINDS.values()]
    scratch += [pltpu.VMEM((2, 4, r, c), F32) for r, c, _ in KINDS.values()]
    scratch += [pltpu.VMEM((2048, 768), BF16), pltpu.VMEM((2048, 768), BF16), pltpu.VMEM((1024, 3072), BF16), pltpu.VMEM((4, NDEV, 16, 128), F32)]
    dma = pltpu.SemaphoreType.DMA
    scratch += [dma((21,)), dma((14,)), dma((4, 10)), dma((4, 10)), dma((4, 9)), dma((4, 9)), dma((4, 10)), dma((4, 10)), dma((4,)), dma((4,))]
    shapes = [jax.ShapeDtypeStruct(s.shape, F32) for s in states[2:]] + [jax.ShapeDtypeStruct(x_next.shape, BF16)]
    any_spec = pl.BlockSpec(memory_space=pl.ANY)
    return pl.pallas_call(
        step_kernel,
        out_shape=shapes,
        in_specs=[any_spec] * 13,
        out_specs=[any_spec] * 7,
        scratch_shapes=scratch,
        compiler_params=pltpu.CompilerParams(collective_id=0, has_side_effects=True, vmem_limit_bytes=66_000_000),
        cost_estimate=pl.CostEstimate(flops=4 * 2 * 2048 * 768 * 3072, bytes_accessed=60_000_000, transcendentals=0),
        name='reduce_update_gather_forward',
    )(*parts, *states, x_next)


def layer_backward(x_cur, d_cur, w_up_l, w_down_l, need_dx):
    pre_act = jnp.einsum('bsd,df->bsf', x_cur, w_up_l, preferred_element_type=jnp.float32)
    act_f32, gelu_vjp = jax.vjp(jax.nn.gelu, pre_act)
    act_bf = act_f32.astype(jnp.bfloat16)
    d_act = jnp.einsum('bsd,fd->bsf', d_cur, w_down_l, preferred_element_type=jnp.float32)
    d_pre = gelu_vjp(d_act)[0].astype(jnp.bfloat16)
    part_down = jnp.einsum('bsf,bsd->fd', act_bf, d_cur, preferred_element_type=jnp.float32).astype(jnp.bfloat16)
    part_up = jnp.einsum('bsd,bsf->df', x_cur, d_pre, preferred_element_type=jnp.float32).astype(jnp.bfloat16)
    d_next = None
    if need_dx:
        d_next = (d_cur.astype(jnp.float32) + jnp.einsum('bsf,df->bsd', d_pre, w_up_l, preferred_element_type=jnp.float32)).astype(jnp.bfloat16)
    return part_up, part_down, d_next


def solution(mesh):
    shard_rows = P(None, 'fsdp')
    shard_batch = P('fsdp')
    spec_whole = P()

    def local_step(x_layers, dy_top, x_next, w_up, w_down, acc_up, acc_down, master_up, master_down, mom_up, mom_down, var_up, var_down):
        layers = w_up.shape[0]
        parts = [None] * layers
        d_cur = dy_top
        for layer_id in reversed(range(layers)):
            part_up, part_down, d_cur = layer_backward(x_layers[layer_id], d_cur, w_up[layer_id], w_down[layer_id], layer_id > 0)
            parts[layer_id] = (part_up.reshape(2, 2, 2, 2, 48, 3072), part_down.reshape(2, 2, 2, 2, 192, 768))
        states = (acc_up, acc_down, master_up, master_down, mom_up, mom_down, var_up, var_down)
        return tuple(gather_step(parts[0] + parts[1], states, x_next))

    return jax.shard_map(local_step, mesh=mesh, in_specs=(shard_rows, shard_batch, shard_batch, spec_whole, spec_whole) + (shard_rows,) * 8, out_specs=(shard_rows,) * 6 + (shard_batch,), check_vma=False)
```

```python
import functools

import jax
import jax.numpy as jnp
from jax import lax
from jax.experimental import pallas as pl
from jax.experimental.pallas import tpu as pltpu
from jax.sharding import PartitionSpec as P

MICRO_STEPS = 2
STEP_COUNT = 3
BETA_MOM = 0.9
BETA_VAR = 0.999
ADAM_EPS = 1e-6
WEIGHT_DECAY = 0.01
LEARN_RATE = 0.06
NDEV = 16
D, FF, TOK = 768, 3072, 2048
TILES = FF // D
MT = 512
PAIR = 384
UP_ROWS, DN_ROWS = D // NDEV, FF // NDEV
LANES, SUB = 128, 8
MESH = pl.DeviceIdType.MESH
F32 = jnp.float32
BF16 = jnp.bfloat16
HBM = pl.BlockSpec(memory_space=pl.ANY)
DMA = pltpu.SemaphoreType.DMA
ALL = slice(None)

KINDS = {'up': (UP_ROWS, FF, MT, TILES), 'dn': (DN_ROWS, D, D, 1)}
MATRIX = {('up', 0): 0, ('dn', 0): 1, ('up', 1): 2, ('dn', 1): 3}
DIM_ORDERS = ((0, 1, 2), (1, 2, 0), (2, 0, 1))
GELU_A, GELU_B = 0.7978845608028654, 0.035677408136300125
ROW_COL = (((1,), (1,)), ((), ()))
COL_COL = (((0,), (0,)), ((), ()))


def span(i, n):
    return pl.ds(pl.multiple_of(i * n, n), n)


def gelu_tanh(v):
    half = 0.5 * v
    return half + half * jnp.tanh(v * (GELU_A + GELU_B * (v * v)))


def gelu_parts(v):
    sq = v * v
    t = jnp.tanh(v * (GELU_A + GELU_B * sq))
    half = 0.5 + 0.5 * t
    slope = 0.5 * v * (1.0 - t * t) * (GELU_A + (3 * GELU_B) * sq)
    return v * half, half + slope


def step_kernel(*refs):
    (x_all, dy_hbm, x_hbm, w_up, w_dn, acc_up, acc_dn, mas_up, mas_dn, mom_up, mom_dn, var_up, var_dn,
     o_mas_up, o_mas_dn, o_mom_up, o_mom_dn, o_var_up, o_var_dn, o_x, o_wu, o_wd,
     wu, wd, r0u, r0d, q1u, q1d, q2u, q2d, q3u, q3d, stu, std, xa, dy, xb, ta, td, w1t, w2t, norms,
     ld_sem, x_sem, wt_sem, out_sem, w_sem, xo_sem, rs_send, rs_recv, ag_send, ag_recv, dd_send, dd_recv, nm_send, nm_recv) = refs
    whole = {'up': wu, 'dn': wd}
    recv0 = {'up': r0u, 'dn': r0d}
    recvs = {'up': (q1u, q2u, q3u), 'dn': (q1d, q2d, q3d)}
    state_in = {'up': (acc_up, mas_up, mom_up, var_up), 'dn': (acc_dn, mas_dn, mom_dn, var_dn)}
    state_out = {'up': (None, o_mas_up, o_mom_up, o_var_up), 'dn': (None, o_mas_dn, o_mom_dn, o_var_dn)}
    w_out = {'up': o_wu, 'dn': o_wd}

    me = lax.axis_index('fsdp')
    bits = (me // 8, (me // 4) % 2, (me // 2) % 2)
    core = me % 2
    partner = me + 1 - 2 * core
    neighbours = tuple(me + step * (1 - 2 * bit) for bit, step in zip(bits, (8, 4, 2)))

    def local(src, dst, sem):
        return pltpu.make_async_copy(src, dst, sem)

    def remote(src, dst, send, recv, device):
        return pltpu.make_async_remote_copy(src_ref=src, dst_ref=dst, send_sem=send, recv_sem=recv, device_id=(device,), device_id_type=MESH)

    def st_block(kind, layer, k):
        if kind == 'up':
            return stu.at[layer, k]
        return std.at[span(4 * layer + k, DN_ROWS)]

    def state_loads(kind, layer):
        return [local(state_in[kind][k].at[layer], st_block(kind, layer, k), ld_sem.at[MATRIX[kind, layer], k]) for k in range(4)]

    def state_store(kind, layer, k):
        return local(st_block(kind, layer, k), state_out[kind][k].at[layer], out_sem.at[MATRIX[kind, layer], k])

    def w_store(kind):
        return local(whole[kind].at[1], w_out[kind], w_sem.at[MATRIX[kind, 0]])

    x1_load = local(x_all.at[1, 0], xa, x_sem.at[0])
    dy_load = local(dy_hbm.at[0], dy, x_sem.at[1])
    x0_load = local(x_all.at[0, 0], xb, x_sem.at[2])
    xn_load = local(x_hbm.at[0], xa, x_sem.at[3])

    def tile_loads(t):
        layer, cols, slot = 1 - t // TILES, span(t % TILES, D), t % 2
        return (local(w_up.at[layer, :, cols], w1t.at[slot], wt_sem.at[0, slot]),
                local(w_dn.at[layer, cols], w2t.at[slot], wt_sem.at[1, slot]))

    def start(copies):
        for copy in copies:
            copy.start()

    def wait(copies):
        for copy in copies:
            copy.wait()

    start((x1_load,) + tile_loads(0) + (dy_load, x0_load))
    start(state_loads('up', 1) + state_loads('up', 0))

    barrier = pltpu.get_barrier_semaphore()

    def hello(k, carry):
        pl.semaphore_signal(barrier, inc=1, device_id=(lax.rem(me + k, NDEV),), device_id_type=MESH)
        return carry

    lax.fori_loop(1, NDEV, hello, 0)
    pl.semaphore_wait(barrier, NDEV - 1)

    def place(fixed):
        return tuple(fixed.get(d, ALL) for d in range(3))

    def rs_core(kind, layer, k):
        m, cols = MATRIX[kind, layer], span(k, D)
        return remote(whole[kind].at[layer, :, :, :, 1 - core, :, cols], recv0[kind].at[:, :, :, :, cols], rs_send.at[m, k, 0], rs_recv.at[m, k, 0], partner)

    def rs_copies(kind, layer, stage, k):
        m, cols, third = MATRIX[kind, layer], span(k, D), KINDS[kind][0] // 3
        copies = []
        for p, dims in enumerate(DIM_ORDERS):
            fixed = {d: bits[d] for d in dims[:stage]}
            fixed[dims[stage]] = 1 - bits[dims[stage]]
            src = recv0[kind].at[place(fixed) + (pl.ds(third * p, third), cols)]
            dst = recvs[kind][stage].at[(p,) + (ALL,) * (3 - stage) + (cols,)]
            sem = 1 + 3 * stage + p
            copies.append(remote(src, dst, rs_send.at[m, k, sem], rs_recv.at[m, k, sem], neighbours[dims[stage]]))
        return copies

    def rs_begin(kind, layer, k=0):
        rs_core(kind, layer, k).start()

    def rs_first(kind, layer, k=0):
        rs_core(kind, layer, k).wait()
        cols = span(k, D)

        def add(i, carry):
            z, y, x = i // 4, (i // 2) % 2, i % 2
            recv0[kind][z, y, x, :, cols] = recv0[kind][z, y, x, :, cols] + whole[kind][layer, z, y, x, core, :, cols]
            return carry

        lax.fori_loop(0, 8, add, 0)
        start(rs_copies(kind, layer, 0, k))

    def rs_next(kind, layer, stage, k=0):
        cols, third = span(k, D), KINDS[kind][0] // 3
        buf, got = recv0[kind], recvs[kind][stage]
        arriving = rs_copies(kind, layer, stage, k)
        for p, dims in enumerate(DIM_ORDERS):
            arriving[p].wait()
            free = [d for d in range(3) if d in dims[stage + 1:]]
            for i in range(2 ** len(free)):
                where = {d: bits[d] for d in dims[:stage + 1]}
                slot = []
                for j, d in enumerate(free):
                    where[d] = (i >> (len(free) - 1 - j)) & 1
                    slot.append(where[d])
                idx = place(where) + (pl.ds(third * p, third), cols)
                buf[idx] = buf[idx] + got[(p,) + tuple(slot) + (ALL, cols)]
        start(rs_copies(kind, layer, stage + 1, k))

    def lamb(kind, layer):
        m = MATRIX[kind, layer]
        rows, cols, wide, chunks = KINDS[kind]
        third, per_row = rows // 3, cols // wide
        buf, got = recv0[kind], recvs[kind][2]
        st = functools.partial(st_block, kind, layer)
        wait(state_loads(kind, layer))
        for k in range(chunks):
            wait(rs_copies(kind, layer, 2, k))
        zero = jnp.zeros((2 * SUB, wide), F32)
        w_sum, u_sum = zero, zero
        for p in range(3):
            def chunk(i, carry):
                w_acc, u_acc = carry
                row, cs = i // per_row, span(i % per_row, wide)
                near = span(row, 2 * SUB)
                at = (pl.ds(pl.multiple_of(third * p + row * 2 * SUB, 2 * SUB), 2 * SUB), cs)
                total = buf[bits + at].astype(F32) + got[p, near, cs].astype(F32)
                master = st(1)[at]
                grad = (st(0)[at] + total) / MICRO_STEPS
                mom = BETA_MOM * st(2)[at] + (1.0 - BETA_MOM) * grad
                var = BETA_VAR * st(3)[at] + (1.0 - BETA_VAR) * grad * grad
                upd = (mom / (1.0 - BETA_MOM ** STEP_COUNT)) / (jnp.sqrt(var / (1.0 - BETA_VAR ** STEP_COUNT)) + ADAM_EPS) + WEIGHT_DECAY * master
                st(0)[at] = upd
                st(2)[at] = mom
                st(3)[at] = var
                return w_acc + master * master, u_acc + upd * upd

            w_sum, u_sum = lax.fori_loop(0, (third // (2 * SUB)) * per_row, chunk, (w_sum, u_sum))

        def fold(v):
            tiles = [v[SUB * i:SUB * i + SUB, LANES * j:LANES * j + LANES] for i in range(2) for j in range(wide // LANES)]
            return functools.reduce(lambda a, b: a + b, tiles)

        norms[m, me, 0:SUB] = fold(w_sum)
        norms[m, me, SUB:2 * SUB] = fold(u_sum)
        start([state_store(kind, layer, k) for k in (2, 3)])

        def tell(k, carry):
            remote(norms.at[m, me], norms.at[m, me], nm_send.at[m], nm_recv.at[m], lax.rem(me + k, NDEV)).start()
            return carry

        lax.fori_loop(1, NDEV, tell, 0)

    def apply(kind, layer):
        m = MATRIX[kind, layer]
        rows, cols, wide, _ = KINDS[kind]
        st = functools.partial(st_block, kind, layer)
        others = norms.at[m, pl.ds(0, NDEV - 1)]
        wait([local(others, others, sem.at[m]) for sem in (nm_send, nm_recv)])
        sums = jnp.sum(norms[m], axis=0)
        total = [jnp.sum(jnp.sum(v, axis=0, keepdims=True), axis=1, keepdims=True) for v in (sums[0:SUB], sums[SUB:2 * SUB])]
        scale = LEARN_RATE * (jnp.sqrt(total[0]) / jnp.sqrt(total[1]))
        per_row = cols // wide

        def chunk(i, carry):
            at = (span(i // per_row, 2 * SUB), span(i % per_row, wide))
            new = st(1)[at] - scale * st(0)[at]
            st(1)[at] = new
            whole[kind][(layer,) + bits + (core,) + at] = new.astype(BF16)
            return carry

        lax.fori_loop(0, (rows // (2 * SUB)) * per_row, chunk, 0)
        state_store(kind, layer, 1).start()

    def ag_copies(kind, layer, stage):
        m, third = MATRIX[kind, layer], KINDS[kind][0] // 3
        copies = []
        for p, dims in enumerate(DIM_ORDERS):
            ref = whole[kind].at[(layer,) + place({d: bits[d] for d in dims[:3 - stage]}) + (core, pl.ds(third * p, third))]
            copies.append(remote(ref, ref, ag_send.at[m, stage, p], ag_recv.at[m, stage, p], neighbours[dims[2 - stage]]))
        return copies

    def own_pass(kind, layer):
        m = MATRIX[kind, layer]
        ref = whole[kind].at[(layer,) + bits + (core,)]
        return remote(ref, ref, dd_send.at[m, 3, 0], dd_recv.at[m, 3, 0], partner)

    def pass_copies(kind, layer, stage):
        m, third = MATRIX[kind, layer], KINDS[kind][0] // 3
        copies = []
        for p, dims in enumerate(DIM_ORDERS):
            fixed = {d: bits[d] for d in dims[:2 - stage]}
            fixed[dims[2 - stage]] = 1 - bits[dims[2 - stage]]
            ref = whole[kind].at[(layer,) + place(fixed) + (core, pl.ds(third * p, third))]
            copies.append(remote(ref, ref, dd_send.at[m, stage, p], dd_recv.at[m, stage, p], partner))
        return copies

    def ag_begin(kind, layer):
        start(ag_copies(kind, layer, 0))
        own_pass(kind, layer).start()

    def ag_next(kind, layer, stage):
        wait(ag_copies(kind, layer, stage))
        if stage < 2:
            start(ag_copies(kind, layer, stage + 1))
        start(pass_copies(kind, layer, stage))

    def ag_end(kind, layer):
        own_pass(kind, layer).wait()
        for stage in range(3):
            wait(pass_copies(kind, layer, stage))
        if layer == 1:
            w_store(kind).start()

    def hidden(x_ref, slot):
        def rows(i, carry):
            at = span(i, MT)
            pre = jnp.dot(x_ref[at, :], w1t[slot], preferred_element_type=F32)
            d_act = lax.dot_general(dy[at, :], w2t[slot], ROW_COL, preferred_element_type=F32)
            a, slope = gelu_parts(pre)
            ta[at, :] = a.astype(BF16)
            td[at, :] = (d_act * slope).astype(BF16)
            return carry

        lax.fori_loop(0, TOK // MT, rows, 0)

    def part_down(layer, f):
        def chunk(j, carry):
            out = lax.dot_general(ta[:, span(j, PAIR)], dy[...], COL_COL, preferred_element_type=F32)
            wd[layer, f // 2, f % 2, j] = out.astype(BF16).reshape(2, DN_ROWS, D)
            return carry

        lax.fori_loop(0, 2, chunk, 0)

    def part_up(layer, f, x_ref):
        def chunk(j, carry):
            out = lax.dot_general(x_ref[:, span(j, PAIR)], td[...], COL_COL, preferred_element_type=F32)
            wu[layer, j, :, :, :, :, span(f, D)] = out.astype(BF16).reshape(2, 2, 2, UP_ROWS, D)
            return carry

        lax.fori_loop(0, 2, chunk, 0)

    def back_input(slot):
        def rows(i, carry):
            at = span(i, MT)
            std[at, :] += lax.dot_general(td[at, :], w1t[slot], ROW_COL, preferred_element_type=F32)
            return carry

        lax.fori_loop(0, TOK // MT, rows, 0)

    def clear(i, carry):
        std[span(i, 64), :] = jnp.zeros((64, D), F32)
        return carry

    lax.fori_loop(0, TOK // 64, clear, 0)
    wait((x1_load, dy_load))

    def upper(f, carry):
        slot = f % 2
        wait(tile_loads(f))
        start(tile_loads(f + 1))
        hidden(xa, slot)

        @pl.when(f > 0)
        def _():
            rs_next('up', 1, 0, f - 1)

        part_up(1, f, xa)
        rs_begin('up', 1, f)
        part_down(1, f)
        rs_first('up', 1, f)

        @pl.when(f > 0)
        def _():
            rs_next('up', 1, 1, f - 1)

        back_input(slot)
        return carry

    lax.fori_loop(0, TILES, upper, 0)
    rs_begin('dn', 1)
    xn_load.start()

    def next_dy(i, carry):
        at = span(i, 64)
        dy[at, :] = (dy[at, :].astype(F32) + std[at, :]).astype(BF16)
        return carry

    lax.fori_loop(0, TOK // 64, next_dy, 0)
    rs_next('up', 1, 0, TILES - 1)
    start(state_loads('dn', 1) + state_loads('dn', 0))
    x0_load.wait()

    after_hidden = (
        lambda: (rs_next('up', 1, 1, TILES - 1), rs_first('dn', 1)),
        lambda: rs_next('dn', 1, 0),
        lambda: (rs_next('dn', 1, 1), ag_next('up', 1, 1)),
        lambda: apply('dn', 1),
    )
    after_down = (
        lambda: lamb('up', 1),
        lambda: ag_next('up', 1, 0),
        lambda: lamb('dn', 1),
        lambda: rs_begin('dn', 0),
    )
    after_up = (
        lambda: (apply('up', 1), ag_begin('up', 1)),
        None,
        None,
        lambda: ag_next('up', 1, 2),
    )

    def at_tile(f, steps):
        for k, step in enumerate(steps):
            if step is not None:
                @pl.when(f == k)
                def _(step=step):
                    step()

    def lower(f, carry):
        wait(tile_loads(TILES + f))

        @pl.when(f < TILES - 1)
        def _():
            start(tile_loads(TILES + 1 + f))

        hidden(xb, f % 2)

        @pl.when(f > 0)
        def _():
            rs_first('up', 0, f - 1)

        at_tile(f, after_hidden)
        part_down(0, f)

        @pl.when(f > 0)
        def _():
            rs_next('up', 0, 0, f - 1)

        at_tile(f, after_down)
        part_up(0, f, xb)

        @pl.when(f > 0)
        def _():
            rs_next('up', 0, 1, f - 1)

        at_tile(f, after_up)
        rs_begin('up', 0, f)
        return carry

    lax.fori_loop(0, TILES, lower, 0)
    last = TILES - 1
    rs_first('up', 0, last)
    rs_next('up', 0, 0, last)
    rs_first('dn', 0)
    rs_next('up', 0, 1, last)
    lamb('up', 0)
    ag_end('up', 1)
    rs_next('dn', 0, 0)
    apply('up', 0)
    ag_begin('up', 0)
    rs_next('dn', 0, 1)
    ag_next('up', 0, 0)
    lamb('dn', 0)
    ag_next('up', 0, 1)
    apply('dn', 0)
    ag_begin('dn', 0)
    ag_next('up', 0, 2)
    ag_next('dn', 0, 0)
    ag_end('up', 0)

    xn_load.wait()

    def up_part(base, act):
        def body(n, carry):
            w = wu[0, :, :, :, :, :, span(n, D)].reshape(D, D)
            pre = jnp.dot(xa[base:base + MT, :], w, preferred_element_type=F32)
            act[span(n, MT), :] = gelu_tanh(pre).astype(BF16)
            return carry

        lax.fori_loop(0, TILES, body, 0)

    def down_part(base, act):
        def body(i, carry):
            at = pl.ds(pl.multiple_of(base + i * 256, 256), 256)
            prod = None
            for n in range(TILES):
                w = wd[0, n // 2, n % 2].reshape(D, D)
                term = jnp.dot(act[pl.ds(pl.multiple_of(n * MT + i * 256, 256), 256), :], w, preferred_element_type=F32)
                prod = term if prod is None else prod + term
            xb[at, :] = (xa[at, :].astype(F32) + prod).astype(BF16)
            return carry

        lax.fori_loop(0, 2, body, 0)

    def x_store(half):
        rows = pl.ds(half * 2 * MT, 2 * MT)
        return local(xb.at[rows], o_x.at[rows], xo_sem.at[half])

    up_part(0, ta)
    ag_next('dn', 0, 1)
    up_part(MT, td)
    ag_next('dn', 0, 2)
    ag_begin('dn', 1)
    ag_end('dn', 0)
    down_part(0, ta)
    ag_next('dn', 1, 0)
    down_part(MT, td)
    ag_next('dn', 1, 1)
    x_store(0).start()
    up_part(2 * MT, ta)
    up_part(3 * MT, td)
    ag_next('dn', 1, 2)
    down_part(2 * MT, ta)
    ag_end('dn', 1)
    down_part(3 * MT, td)
    x_store(1).start()
    wait([x_store(0), x_store(1), w_store('up'), w_store('dn')])
    for kind, layer in MATRIX:
        wait([state_store(kind, layer, k) for k in (1, 2, 3)])


def last_layer_kernel(x1, w_up, w_dn, *refs):
    ins, outs = refs[:6], refs[6:12]
    o_x, xv, xo, wu, wd, act, s0, s1, s2, s3, s4, s5, x_sem, w_sem, in_sem, out_sem = refs[12:]
    held = (s0, s1, s2, s3, s4, s5)
    first = pltpu.make_async_copy(x1, xv, x_sem.at[0])
    first.start()
    ups = [pltpu.make_async_copy(w_up.at[:, pl.ds(n * D, D)], wu.at[:, pl.ds(n * D, D)], w_sem.at[n]) for n in range(TILES)]
    downs = [pltpu.make_async_copy(w_dn.at[pl.ds(n * D, D)], wd.at[pl.ds(n * D, D)], w_sem.at[4 + n]) for n in range(TILES)]
    gets = [pltpu.make_async_copy(i, h, in_sem.at[k]) for k, (i, h) in enumerate(zip(ins, held))]
    puts = [pltpu.make_async_copy(h, o, out_sem.at[k]) for k, (h, o) in enumerate(zip(held, outs))]
    for copy in ups + downs + gets:
        copy.start()
    first.wait()
    for n in range(TILES):
        ups[n].wait()

        def rows(i, carry):
            at = span(i, MT)
            pre = jnp.dot(xv[at, :], wu[:, n * D:n * D + D], preferred_element_type=F32)
            act[at, n * D:n * D + D] = gelu_tanh(pre).astype(BF16)
            return carry

        lax.fori_loop(0, 4, rows, 0)
    for get, put in zip(gets, puts):
        get.wait()
        put.start()
    for copy in downs:
        copy.wait()
    sends = []
    for half in range(2):
        def body(i, carry):
            at = pl.ds(pl.multiple_of(half * 2 * MT + i * 256, 256), 256)
            out = jnp.dot(act[at, :], wd[...], preferred_element_type=F32)
            xo[at, :] = (xv[at, :].astype(F32) + out).astype(BF16)
            return carry

        lax.fori_loop(0, 4, body, 0)
        copy = pltpu.make_async_copy(xo.at[pl.ds(half * 2 * MT, 2 * MT)], o_x.at[0, pl.ds(half * 2 * MT, 2 * MT)], out_sem.at[6 + half])
        copy.start()
        sends.append(copy)
    for copy in puts + sends:
        copy.wait()


def whole_step(x_layers, dy_top, x_next, w_up, w_down, *states):
    cores = (2, 2, 2)
    sizes = [(r, c) for r, c, *_ in KINDS.values()]
    scratch = [pltpu.VMEM((2,) + cores + (2, r, c), BF16) for r, c in sizes]
    scratch += [pltpu.VMEM(cores + (r, c), BF16) for r, c in sizes]
    scratch += [pltpu.VMEM((3, 2, 2, r // 3, c), BF16) for r, c in sizes]
    scratch += [pltpu.VMEM((3, 2, r // 3, c), BF16) for r, c in sizes]
    scratch += [pltpu.VMEM((3, r // 3, c), BF16) for r, c in sizes]
    scratch += [pltpu.VMEM((2, 4, UP_ROWS, FF), F32), pltpu.VMEM((TOK, D), F32)]
    scratch += [pltpu.VMEM((TOK, D), BF16)] * 5
    scratch += [pltpu.VMEM((2, D, D), BF16)] * 2 + [pltpu.VMEM((4, NDEV, 16, 128), F32)]
    sem4 = (4, 4)
    rs_sem, ag_sem = DMA((4, TILES, 10)), DMA((4, 4, 3))
    scratch += [DMA(sem4), DMA((4,)), DMA(cores[1:]), DMA(sem4), DMA((2,)), DMA((2,)), rs_sem, rs_sem, ag_sem, ag_sem, ag_sem, ag_sem, DMA((4,)), DMA((4,))]
    state_shapes = [jax.ShapeDtypeStruct(s.shape, F32) for s in states[2:]]
    shapes = state_shapes + [jax.ShapeDtypeStruct((TOK, D), BF16)]
    shapes += [jax.ShapeDtypeStruct(cores + (2, r, c), BF16) for r, c in sizes]
    product = 2 * TOK * D * FF
    res = pl.pallas_call(
        step_kernel,
        out_shape=shapes,
        in_specs=[HBM] * 13,
        out_specs=[HBM] * 9,
        scratch_shapes=scratch,
        compiler_params=pltpu.CompilerParams(collective_id=0, has_side_effects=True, vmem_limit_bytes=67_000_000),
        cost_estimate=pl.CostEstimate(flops=11 * product, bytes_accessed=80_000_000, transcendentals=0),
        name='backward_update_gather',
    )(x_layers, dy_top, x_next, w_up, w_down, *states)
    x_mid, new_up, new_dn = res[6:]
    held = [pltpu.VMEM(s.shape, F32) for s in state_shapes]
    return pl.pallas_call(
        last_layer_kernel,
        out_shape=state_shapes + [jax.ShapeDtypeStruct(x_next.shape, BF16)],
        in_specs=[HBM] * 9,
        out_specs=[HBM] * 7,
        scratch_shapes=[pltpu.VMEM((TOK, D), BF16)] * 2 + [pltpu.VMEM((D, FF), BF16), pltpu.VMEM((FF, D), BF16), pltpu.VMEM((TOK, FF), BF16)] + held + [DMA((1,)), DMA((8,)), DMA((6,)), DMA((8,))],
        compiler_params=pltpu.CompilerParams(vmem_limit_bytes=60_000_000),
        cost_estimate=pl.CostEstimate(flops=2 * product, bytes_accessed=40_000_000, transcendentals=0),
        name='last_layer_forward',
    )(x_mid, new_up.reshape(D, FF), new_dn.reshape(FF, D), *res[:6])


def solution(mesh):
    shard_rows = P(None, 'fsdp')
    shard_batch = P('fsdp')
    spec_whole = P()

    def local_step(*args):
        return tuple(whole_step(*args))

    return jax.shard_map(local_step, mesh=mesh, in_specs=(shard_rows, shard_batch, shard_batch, spec_whole, spec_whole) + (shard_rows,) * 8, out_specs=(shard_rows,) * 6 + (shard_batch,), check_vma=False)
```

```python
import functools

import jax
import jax.numpy as jnp
from jax import lax
from jax.experimental import pallas as pl
from jax.experimental.pallas import tpu as pltpu
from jax.sharding import PartitionSpec as P

MICRO_STEPS = 2
STEP_COUNT = 3
BETA_MOM = 0.9
BETA_VAR = 0.999
ADAM_EPS = 1e-6
WEIGHT_DECAY = 0.01
LEARN_RATE = 0.06
NDEV = 16
D, FF, TOK = 768, 3072, 2048
TILES = FF // D
MT = 512
PAIR = 384
UP_ROWS, DN_ROWS = D // NDEV, FF // NDEV
LANES, SUB = 128, 8
MESH = pl.DeviceIdType.MESH
F32 = jnp.float32
BF16 = jnp.bfloat16
HBM = pl.BlockSpec(memory_space=pl.ANY)
DMA = pltpu.SemaphoreType.DMA
ALL = slice(None)

KINDS = {'up': (UP_ROWS, FF, MT, TILES), 'dn': (DN_ROWS, D, D, 2)}
MATRIX = {('up', 0): 0, ('dn', 0): 1, ('up', 1): 2, ('dn', 1): 3}
DIM_ORDERS = ((0, 1, 2), (1, 2, 0), (2, 0, 1))
GELU_A, GELU_B = 0.7978845608028654, 0.035677408136300125
ROW_COL = (((1,), (1,)), ((), ()))
COL_COL = (((0,), (0,)), ((), ()))


def span(i, n):
    return pl.ds(pl.multiple_of(i * n, n), n)


def gelu_tanh(v):
    half = 0.5 * v
    return half + half * jnp.tanh(v * (GELU_A + GELU_B * (v * v)))


def gelu_parts(v):
    sq = v * v
    t = jnp.tanh(v * (GELU_A + GELU_B * sq))
    half = 0.5 + 0.5 * t
    slope = 0.5 * v * (1.0 - t * t) * (GELU_A + (3 * GELU_B) * sq)
    return v * half, half + slope


def step_kernel(*refs):
    (x_all, dy_hbm, x_hbm, w_up, w_dn, acc_up, acc_dn, mas_up, mas_dn, mom_up, mom_dn, var_up, var_dn,
     o_mas_up, o_mas_dn, o_mom_up, o_mom_dn, o_var_up, o_var_dn, o_x, o_wu, o_wd,
     wu, wd, r0u, r0d, q1u, q1d, q2u, q2d, q3u, q3d, stu, std, xa, dy, xb, ta, td, w1t, w2t, norms,
     ld_sem, x_sem, wt_sem, out_sem, w_sem, xo_sem, rs_send, rs_recv, ag_send, ag_recv, dd_send, dd_recv, nm_send, nm_recv) = refs
    whole = {'up': wu, 'dn': wd}
    recv0 = {'up': r0u, 'dn': r0d}
    recvs = {'up': (q1u, q2u, q3u), 'dn': (q1d, q2d, q3d)}
    state_in = {'up': (acc_up, mas_up, mom_up, var_up), 'dn': (acc_dn, mas_dn, mom_dn, var_dn)}
    state_out = {'up': (None, o_mas_up, o_mom_up, o_var_up), 'dn': (None, o_mas_dn, o_mom_dn, o_var_dn)}
    w_out = {'up': o_wu, 'dn': o_wd}

    me = lax.axis_index('fsdp')
    bits = (me // 8, (me // 4) % 2, (me // 2) % 2)
    core = me % 2
    partner = me + 1 - 2 * core
    neighbours = tuple(me + step * (1 - 2 * bit) for bit, step in zip(bits, (8, 4, 2)))

    def local(src, dst, sem):
        return pltpu.make_async_copy(src, dst, sem)

    def remote(src, dst, send, recv, device):
        return pltpu.make_async_remote_copy(src_ref=src, dst_ref=dst, send_sem=send, recv_sem=recv, device_id=(device,), device_id_type=MESH)

    def st_block(kind, layer, k):
        if kind == 'up':
            return stu.at[layer, k]
        return std.at[span(4 * layer + k, DN_ROWS)]

    def state_loads(kind, layer):
        return [local(state_in[kind][k].at[layer], st_block(kind, layer, k), ld_sem.at[MATRIX[kind, layer], k]) for k in range(4)]

    def state_store(kind, layer, k):
        return local(st_block(kind, layer, k), state_out[kind][k].at[layer], out_sem.at[MATRIX[kind, layer], k])

    def w_store(kind):
        return local(whole[kind].at[1], w_out[kind], w_sem.at[MATRIX[kind, 0]])

    x1_load = local(x_all.at[1, 0], xa, x_sem.at[0])
    dy_load = local(dy_hbm.at[0], dy, x_sem.at[1])
    x0_load = local(x_all.at[0, 0], xb, x_sem.at[2])
    xn_load = local(x_hbm.at[0], xa, x_sem.at[3])

    def tile_loads(t):
        layer, cols, slot = 1 - t // TILES, span(t % TILES, D), t % 2
        return (local(w_up.at[layer, :, cols], w1t.at[slot], wt_sem.at[0, slot]),
                local(w_dn.at[layer, cols], w2t.at[slot], wt_sem.at[1, slot]))

    def start(copies):
        for copy in copies:
            copy.start()

    def wait(copies):
        for copy in copies:
            copy.wait()

    start((x1_load,) + tile_loads(0) + (dy_load, x0_load))
    start(state_loads('up', 1) + state_loads('up', 0))

    barrier = pltpu.get_barrier_semaphore()

    def hello(k, carry):
        pl.semaphore_signal(barrier, inc=1, device_id=(lax.rem(me + k, NDEV),), device_id_type=MESH)
        return carry

    lax.fori_loop(1, NDEV, hello, 0)
    pl.semaphore_wait(barrier, NDEV - 1)

    def place(fixed):
        return tuple(fixed.get(d, ALL) for d in range(3))

    def chunk_cols(kind, k):
        return span(k, KINDS[kind][1] // KINDS[kind][3])

    def rs_core(kind, layer, k):
        m, cols = MATRIX[kind, layer], chunk_cols(kind, k)
        return remote(whole[kind].at[layer, :, :, :, 1 - core, :, cols], recv0[kind].at[:, :, :, :, cols], rs_send.at[m, k, 0], rs_recv.at[m, k, 0], partner)

    def rs_copies(kind, layer, stage, k):
        m, cols, third = MATRIX[kind, layer], chunk_cols(kind, k), KINDS[kind][0] // 3
        copies = []
        for p, dims in enumerate(DIM_ORDERS):
            fixed = {d: bits[d] for d in dims[:stage]}
            fixed[dims[stage]] = 1 - bits[dims[stage]]
            src = recv0[kind].at[place(fixed) + (pl.ds(third * p, third), cols)]
            dst = recvs[kind][stage].at[(p,) + (ALL,) * (3 - stage) + (cols,)]
            sem = 1 + 3 * stage + p
            copies.append(remote(src, dst, rs_send.at[m, k, sem], rs_recv.at[m, k, sem], neighbours[dims[stage]]))
        return copies

    def rs_begin(kind, layer, k=0):
        rs_core(kind, layer, k).start()

    def rs_first(kind, layer, k=0):
        rs_core(kind, layer, k).wait()
        cols = chunk_cols(kind, k)

        def add(i, carry):
            z, y, x = i // 4, (i // 2) % 2, i % 2
            recv0[kind][z, y, x, :, cols] = recv0[kind][z, y, x, :, cols] + whole[kind][layer, z, y, x, core, :, cols]
            return carry

        lax.fori_loop(0, 8, add, 0)
        start(rs_copies(kind, layer, 0, k))

    def rs_next(kind, layer, stage, k=0):
        cols, third = chunk_cols(kind, k), KINDS[kind][0] // 3
        buf, got = recv0[kind], recvs[kind][stage]
        arriving = rs_copies(kind, layer, stage, k)
        for p, dims in enumerate(DIM_ORDERS):
            arriving[p].wait()
            free = [d for d in range(3) if d in dims[stage + 1:]]
            for i in range(2 ** len(free)):
                where = {d: bits[d] for d in dims[:stage + 1]}
                slot = []
                for j, d in enumerate(free):
                    where[d] = (i >> (len(free) - 1 - j)) & 1
                    slot.append(where[d])
                idx = place(where) + (pl.ds(third * p, third), cols)
                buf[idx] = buf[idx] + got[(p,) + tuple(slot) + (ALL, cols)]
        start(rs_copies(kind, layer, stage + 1, k))

    def lamb(kind, layer):
        m = MATRIX[kind, layer]
        rows, cols, wide, chunks = KINDS[kind]
        third, per_row = rows // 3, cols // wide
        buf, got = recv0[kind], recvs[kind][2]
        st = functools.partial(st_block, kind, layer)
        wait(state_loads(kind, layer))
        for k in range(chunks):
            wait(rs_copies(kind, layer, 2, k))
        zero = jnp.zeros((2 * SUB, wide), F32)
        w_sum, u_sum = zero, zero
        for p in range(3):
            def chunk(i, carry):
                w_acc, u_acc = carry
                row, cs = i // per_row, span(i % per_row, wide)
                near = span(row, 2 * SUB)
                at = (pl.ds(pl.multiple_of(third * p + row * 2 * SUB, 2 * SUB), 2 * SUB), cs)
                total = buf[bits + at].astype(F32) + got[p, near, cs].astype(F32)
                master = st(1)[at]
                grad = (st(0)[at] + total) / MICRO_STEPS
                mom = BETA_MOM * st(2)[at] + (1.0 - BETA_MOM) * grad
                var = BETA_VAR * st(3)[at] + (1.0 - BETA_VAR) * grad * grad
                upd = (mom / (1.0 - BETA_MOM ** STEP_COUNT)) / (jnp.sqrt(var / (1.0 - BETA_VAR ** STEP_COUNT)) + ADAM_EPS) + WEIGHT_DECAY * master
                st(0)[at] = upd
                st(2)[at] = mom
                st(3)[at] = var
                return w_acc + master * master, u_acc + upd * upd

            w_sum, u_sum = lax.fori_loop(0, (third // (2 * SUB)) * per_row, chunk, (w_sum, u_sum))

        def fold(v):
            tiles = [v[SUB * i:SUB * i + SUB, LANES * j:LANES * j + LANES] for i in range(2) for j in range(wide // LANES)]
            return functools.reduce(lambda a, b: a + b, tiles)

        norms[m, me, 0:SUB] = fold(w_sum)
        norms[m, me, SUB:2 * SUB] = fold(u_sum)
        start([state_store(kind, layer, k) for k in (2, 3)])

        def tell(k, carry):
            remote(norms.at[m, me], norms.at[m, me], nm_send.at[m], nm_recv.at[m], lax.rem(me + k, NDEV)).start()
            return carry

        lax.fori_loop(1, NDEV, tell, 0)

    def apply(kind, layer):
        m = MATRIX[kind, layer]
        rows, cols, wide, _ = KINDS[kind]
        st = functools.partial(st_block, kind, layer)
        others = norms.at[m, pl.ds(0, NDEV - 1)]
        wait([local(others, others, sem.at[m]) for sem in (nm_send, nm_recv)])
        sums = jnp.sum(norms[m], axis=0)
        total = [jnp.sum(jnp.sum(v, axis=0, keepdims=True), axis=1, keepdims=True) for v in (sums[0:SUB], sums[SUB:2 * SUB])]
        scale = LEARN_RATE * (jnp.sqrt(total[0]) / jnp.sqrt(total[1]))
        per_row = cols // wide

        def chunk(i, carry):
            at = (span(i // per_row, 2 * SUB), span(i % per_row, wide))
            new = st(1)[at] - scale * st(0)[at]
            st(1)[at] = new
            whole[kind][(layer,) + bits + (core,) + at] = new.astype(BF16)
            return carry

        lax.fori_loop(0, (rows // (2 * SUB)) * per_row, chunk, 0)
        state_store(kind, layer, 1).start()

    def ag_copies(kind, layer, stage):
        m, third = MATRIX[kind, layer], KINDS[kind][0] // 3
        copies = []
        for p, dims in enumerate(DIM_ORDERS):
            ref = whole[kind].at[(layer,) + place({d: bits[d] for d in dims[:3 - stage]}) + (core, pl.ds(third * p, third))]
            copies.append(remote(ref, ref, ag_send.at[m, stage, p], ag_recv.at[m, stage, p], neighbours[dims[2 - stage]]))
        return copies

    def own_pass(kind, layer):
        m = MATRIX[kind, layer]
        ref = whole[kind].at[(layer,) + bits + (core,)]
        return remote(ref, ref, dd_send.at[m, 3, 0], dd_recv.at[m, 3, 0], partner)

    def pass_copies(kind, layer, stage):
        m, third = MATRIX[kind, layer], KINDS[kind][0] // 3
        copies = []
        for p, dims in enumerate(DIM_ORDERS):
            fixed = {d: bits[d] for d in dims[:2 - stage]}
            fixed[dims[2 - stage]] = 1 - bits[dims[2 - stage]]
            ref = whole[kind].at[(layer,) + place(fixed) + (core, pl.ds(third * p, third))]
            copies.append(remote(ref, ref, dd_send.at[m, stage, p], dd_recv.at[m, stage, p], partner))
        return copies

    def ag_begin(kind, layer):
        start(ag_copies(kind, layer, 0))
        own_pass(kind, layer).start()

    def ag_next(kind, layer, stage):
        wait(ag_copies(kind, layer, stage))
        if stage < 2:
            start(ag_copies(kind, layer, stage + 1))
        start(pass_copies(kind, layer, stage))

    def ag_end(kind, layer):
        own_pass(kind, layer).wait()
        for stage in range(3):
            wait(pass_copies(kind, layer, stage))
        if layer == 1:
            w_store(kind).start()

    def hidden(x_ref, slot):
        def rows(i, carry):
            at = span(i, MT)
            pre = jnp.dot(x_ref[at, :], w1t[slot], preferred_element_type=F32)
            d_act = lax.dot_general(dy[at, :], w2t[slot], ROW_COL, preferred_element_type=F32)
            a, slope = gelu_parts(pre)
            ta[at, :] = a.astype(BF16)
            td[at, :] = (d_act * slope).astype(BF16)
            return carry

        lax.fori_loop(0, TOK // MT, rows, 0)

    def part_down(layer, f):
        def chunk(j, carry):
            out = lax.dot_general(ta[:, span(j, PAIR)], dy[...], COL_COL, preferred_element_type=F32)
            wd[layer, f // 2, f % 2, j] = out.astype(BF16).reshape(2, DN_ROWS, D)
            return carry

        lax.fori_loop(0, 2, chunk, 0)

    def part_up(layer, f, x_ref):
        def chunk(j, carry):
            out = lax.dot_general(x_ref[:, span(j, PAIR)], td[...], COL_COL, preferred_element_type=F32)
            wu[layer, j, :, :, :, :, span(f, D)] = out.astype(BF16).reshape(2, 2, 2, UP_ROWS, D)
            return carry

        lax.fori_loop(0, 2, chunk, 0)

    def back_input(slot):
        def rows(i, carry):
            at = span(i, MT)
            std[at, :] += lax.dot_general(td[at, :], w1t[slot], ROW_COL, preferred_element_type=F32)
            return carry

        lax.fori_loop(0, TOK // MT, rows, 0)

    def clear(i, carry):
        std[span(i, 64), :] = jnp.zeros((64, D), F32)
        return carry

    lax.fori_loop(0, TOK // 64, clear, 0)
    wait((x1_load, dy_load))

    def upper(f, carry):
        slot = f % 2
        wait(tile_loads(f))
        start(tile_loads(f + 1))
        hidden(xa, slot)

        @pl.when(f > 0)
        def _():
            rs_next('up', 1, 0, f - 1)

        part_up(1, f, xa)
        rs_begin('up', 1, f)
        part_down(1, f)
        back_input(slot)
        rs_first('up', 1, f)

        @pl.when(f > 0)
        def _():
            rs_next('up', 1, 1, f - 1)

        return carry

    lax.fori_loop(0, TILES, upper, 0)
    rs_begin('dn', 1, 0)
    rs_begin('dn', 1, 1)
    xn_load.start()

    def next_dy(i, carry):
        at = span(i, 64)
        dy[at, :] = (dy[at, :].astype(F32) + std[at, :]).astype(BF16)
        return carry

    lax.fori_loop(0, TOK // 64, next_dy, 0)
    start(state_loads('dn', 1) + state_loads('dn', 0))
    x0_load.wait()

    last = TILES - 1
    after_hidden = (
        lambda: rs_next('up', 1, 0, last),
        lambda: rs_next('dn', 1, 1, 0),
        lambda: (rs_first('up', 0, 1), rs_next('dn', 1, 1, 1), ag_next('up', 1, 1)),
        lambda: (rs_first('up', 0, 2), lamb('dn', 1), rs_next('up', 0, 0, 0), rs_next('up', 0, 0, 1)),
    )
    after_down = (
        lambda: (rs_next('up', 1, 1, last), rs_first('dn', 1, 0), lamb('up', 1), rs_next('dn', 1, 0, 0), apply('up', 1)),
        lambda: (rs_next('dn', 1, 0, 1), ag_next('up', 1, 0), rs_first('up', 0, 0)),
        None,
        lambda: (rs_next('up', 0, 0, 2), apply('dn', 1), rs_begin('dn', 0, 0), rs_begin('dn', 0, 1), ag_begin('dn', 1)),
    )
    after_up = (
        lambda: (ag_begin('up', 1), rs_first('dn', 1, 1)),
    )

    def at_tile(f, steps):
        for k, step in enumerate(steps):
            if step is not None:
                @pl.when(f == k)
                def _(step=step):
                    step()

    def lower(f, carry):
        wait(tile_loads(TILES + f))

        @pl.when(f < TILES - 1)
        def _():
            start(tile_loads(TILES + 1 + f))

        hidden(xb, f % 2)
        at_tile(f, after_hidden)
        part_down(0, f)
        at_tile(f, after_down)
        part_up(0, f, xb)
        rs_begin('up', 0, f)
        at_tile(f, after_up)
        return carry

    lax.fori_loop(0, TILES, lower, 0)
    rs_next('up', 0, 1, 0)
    rs_next('up', 0, 1, 1)
    rs_next('up', 0, 1, 2)
    rs_first('dn', 0, 0)
    rs_first('up', 0, last)
    rs_first('dn', 0, 1)
    rs_next('up', 0, 0, last)
    rs_next('dn', 0, 0, 0)
    rs_next('up', 0, 1, last)
    rs_next('dn', 0, 0, 1)
    lamb('up', 0)
    rs_next('dn', 0, 1, 0)
    rs_next('dn', 0, 1, 1)
    apply('up', 0)
    ag_begin('up', 0)
    lamb('dn', 0)
    ag_next('up', 0, 0)
    apply('dn', 0)
    ag_begin('dn', 0)
    ag_next('up', 0, 1)
    ag_next('dn', 0, 0)
    ag_next('up', 0, 2)
    ag_next('dn', 0, 1)
    ag_end('up', 0)

    xn_load.wait()

    def up_part(base, act):
        def body(n, carry):
            w = wu[0, :, :, :, :, :, span(n, D)].reshape(D, D)
            pre = jnp.dot(xa[base:base + MT, :], w, preferred_element_type=F32)
            act[span(n, MT), :] = gelu_tanh(pre).astype(BF16)
            return carry

        lax.fori_loop(0, TILES, body, 0)

    def down_part(base, act):
        def body(i, carry):
            at = pl.ds(pl.multiple_of(base + i * 256, 256), 256)
            prod = None
            for n in range(TILES):
                w = wd[0, n // 2, n % 2].reshape(D, D)
                term = jnp.dot(act[pl.ds(pl.multiple_of(n * MT + i * 256, 256), 256), :], w, preferred_element_type=F32)
                prod = term if prod is None else prod + term
            xb[at, :] = (xa[at, :].astype(F32) + prod).astype(BF16)
            return carry

        lax.fori_loop(0, 2, body, 0)

    def x_store(half):
        rows = pl.ds(half * 2 * MT, 2 * MT)
        return local(xb.at[rows], o_x.at[rows], xo_sem.at[half])

    up_part(0, ta)
    ag_next('up', 1, 2)
    ag_next('dn', 1, 0)
    up_part(MT, td)
    ag_next('dn', 0, 2)
    ag_next('dn', 1, 1)
    ag_end('dn', 0)
    down_part(0, ta)
    down_part(MT, td)
    x_store(0).start()
    up_part(2 * MT, ta)
    ag_end('up', 1)
    up_part(3 * MT, td)
    ag_next('dn', 1, 2)
    down_part(2 * MT, ta)
    down_part(3 * MT, td)
    ag_end('dn', 1)
    x_store(1).start()
    wait([x_store(0), x_store(1), w_store('up'), w_store('dn')])
    for kind, layer in MATRIX:
        wait([state_store(kind, layer, k) for k in (1, 2, 3)])


def last_layer_kernel(x1, w_up, w_dn, *refs):
    ins, outs = refs[:6], refs[6:12]
    o_x, xv, xo, wu, wd, acc, s0, s1, s2, s3, s4, s5, x_sem, w_sem, in_sem, out_sem = refs[12:]
    held = (s0, s1, s2, s3, s4, s5)
    first = pltpu.make_async_copy(x1, xv, x_sem.at[0])
    first.start()
    ups = [pltpu.make_async_copy(w_up.at[:, pl.ds(n * D, D)], wu.at[:, pl.ds(n * D, D)], w_sem.at[n]) for n in range(TILES)]
    downs = [pltpu.make_async_copy(w_dn.at[pl.ds(n * D, D)], wd.at[pl.ds(n * D, D)], w_sem.at[4 + n]) for n in range(TILES)]
    gets = [pltpu.make_async_copy(i, h, in_sem.at[k]) for k, (i, h) in enumerate(zip(ins, held))]
    puts = [pltpu.make_async_copy(h, o, out_sem.at[k]) for k, (h, o) in enumerate(zip(held, outs))]
    for up, down in zip(ups, downs):
        up.start()
        down.start()
    for copy in gets:
        copy.start()
    first.wait()

    def x_store(i):
        return pltpu.make_async_copy(xo.at[span(i, MT)], o_x.at[0, span(i, MT)], out_sem.at[6 + i])

    for n in range(TILES):
        ups[n].wait()
        downs[n].wait()

        def rows(i, carry):
            at, tile = span(i, MT), slice(n * D, n * D + D)
            pre = jnp.dot(xv[at, :], wu[:, tile], preferred_element_type=F32)
            out = jnp.dot(gelu_tanh(pre).astype(BF16), wd[tile, :], preferred_element_type=F32)
            if n == 0:
                acc[at, :] = xv[at, :].astype(F32) + out
            elif n < TILES - 1:
                acc[at, :] += out
            else:
                xo[at, :] = (acc[at, :] + out).astype(BF16)
                x_store(i).start()
            return carry

        lax.fori_loop(0, TOK // MT, rows, 0)
        if n == 1:
            for get, put in zip(gets, puts):
                get.wait()
                put.start()
    for copy in puts + [x_store(i) for i in range(TOK // MT)]:
        copy.wait()


def whole_step(x_layers, dy_top, x_next, w_up, w_down, *states):
    cores = (2, 2, 2)
    sizes = [(r, c) for r, c, *_ in KINDS.values()]
    scratch = [pltpu.VMEM((2,) + cores + (2, r, c), BF16) for r, c in sizes]
    scratch += [pltpu.VMEM(cores + (r, c), BF16) for r, c in sizes]
    scratch += [pltpu.VMEM((3, 2, 2, r // 3, c), BF16) for r, c in sizes]
    scratch += [pltpu.VMEM((3, 2, r // 3, c), BF16) for r, c in sizes]
    scratch += [pltpu.VMEM((3, r // 3, c), BF16) for r, c in sizes]
    scratch += [pltpu.VMEM((2, 4, UP_ROWS, FF), F32), pltpu.VMEM((TOK, D), F32)]
    scratch += [pltpu.VMEM((TOK, D), BF16)] * 5
    scratch += [pltpu.VMEM((2, D, D), BF16)] * 2 + [pltpu.VMEM((4, NDEV, 16, 128), F32)]
    sem4 = (4, 4)
    rs_sem, ag_sem = DMA((4, TILES, 10)), DMA((4, 4, 3))
    scratch += [DMA(sem4), DMA((4,)), DMA(cores[1:]), DMA(sem4), DMA((2,)), DMA((2,)), rs_sem, rs_sem, ag_sem, ag_sem, ag_sem, ag_sem, DMA((4,)), DMA((4,))]
    state_shapes = [jax.ShapeDtypeStruct(s.shape, F32) for s in states[2:]]
    shapes = state_shapes + [jax.ShapeDtypeStruct((TOK, D), BF16)]
    shapes += [jax.ShapeDtypeStruct(cores + (2, r, c), BF16) for r, c in sizes]
    product = 2 * TOK * D * FF
    res = pl.pallas_call(
        step_kernel,
        out_shape=shapes,
        in_specs=[HBM] * 13,
        out_specs=[HBM] * 9,
        scratch_shapes=scratch,
        compiler_params=pltpu.CompilerParams(collective_id=0, has_side_effects=True, vmem_limit_bytes=67_000_000),
        cost_estimate=pl.CostEstimate(flops=11 * product, bytes_accessed=80_000_000, transcendentals=0),
        name='backward_update_gather',
    )(x_layers, dy_top, x_next, w_up, w_down, *states)
    x_mid, new_up, new_dn = res[6:]
    held = [pltpu.VMEM(s.shape, F32) for s in state_shapes]
    return pl.pallas_call(
        last_layer_kernel,
        out_shape=state_shapes + [jax.ShapeDtypeStruct(x_next.shape, BF16)],
        in_specs=[HBM] * 9,
        out_specs=[HBM] * 7,
        scratch_shapes=[pltpu.VMEM((TOK, D), BF16)] * 2 + [pltpu.VMEM((D, FF), BF16), pltpu.VMEM((FF, D), BF16), pltpu.VMEM((TOK, D), F32)] + held + [DMA((1,)), DMA((8,)), DMA((6,)), DMA((10,))],
        compiler_params=pltpu.CompilerParams(vmem_limit_bytes=60_000_000),
        cost_estimate=pl.CostEstimate(flops=2 * product, bytes_accessed=40_000_000, transcendentals=0),
        name='last_layer_forward',
    )(x_mid, new_up.reshape(D, FF), new_dn.reshape(FF, D), *res[:6])


def solution(mesh):
    shard_rows = P(None, 'fsdp')
    shard_batch = P('fsdp')
    spec_whole = P()

    def local_step(*args):
        return tuple(whole_step(*args))

    return jax.shard_map(local_step, mesh=mesh, in_specs=(shard_rows, shard_batch, shard_batch, spec_whole, spec_whole) + (shard_rows,) * 8, out_specs=(shard_rows,) * 6 + (shard_batch,), check_vma=False)
```

```python
import functools

import jax
import jax.numpy as jnp
from jax import lax
from jax.experimental import pallas as pl
from jax.experimental.pallas import tpu as pltpu
from jax.sharding import PartitionSpec as P

MICRO_STEPS = 2
STEP_COUNT = 3
BETA_MOM = 0.9
BETA_VAR = 0.999
ADAM_EPS = 1e-6
WEIGHT_DECAY = 0.01
LEARN_RATE = 0.06
NDEV = 16
D, FF, TOK = 768, 3072, 2048
TILES = FF // D
MT = 512
PAIR = 384
UP_ROWS, DN_ROWS = D // NDEV, FF // NDEV
LANES, SUB = 128, 8
MESH = pl.DeviceIdType.MESH
F32 = jnp.float32
BF16 = jnp.bfloat16
HBM = pl.BlockSpec(memory_space=pl.ANY)
DMA = pltpu.SemaphoreType.DMA
ALL = slice(None)

KINDS = {'up': (UP_ROWS, FF, MT, TILES), 'dn': (DN_ROWS, D, D, 2)}
MATRIX = {('up', 0): 0, ('dn', 0): 1, ('up', 1): 2, ('dn', 1): 3}
DIM_ORDERS = ((0, 1, 2), (1, 2, 0), (2, 0, 1))
GELU_A, GELU_B = 0.7978845608028654, 0.035677408136300125
ROW_COL = (((1,), (1,)), ((), ()))
COL_COL = (((0,), (0,)), ((), ()))


def span(i, n):
    return pl.ds(pl.multiple_of(i * n, n), n)


def gelu_tanh(v):
    half = 0.5 * v
    return half + half * jnp.tanh(v * (GELU_A + GELU_B * (v * v)))


def gelu_parts(v):
    sq = v * v
    t = jnp.tanh(v * (GELU_A + GELU_B * sq))
    half = 0.5 + 0.5 * t
    slope = 0.5 * v * (1.0 - t * t) * (GELU_A + (3 * GELU_B) * sq)
    return v * half, half + slope


def step_kernel(*refs):
    (x_all, dy_hbm, x_hbm, w_up, w_dn, acc_up, acc_dn, mas_up, mas_dn, mom_up, mom_dn, var_up, var_dn,
     o_mas_up, o_mas_dn, o_mom_up, o_mom_dn, o_var_up, o_var_dn, o_x, o_wu, o_wd,
     wu, wd, r0u, r0d, q1u, q1d, q2u, q2d, q3u, q3d, stu, std, xa, dy, xb, ta, td, w1t, w2t, norms,
     ld_sem, x_sem, first_sem, wt_sem, out_sem, w_sem, xo_sem, rs_send, rs_recv, ag_send, ag_recv, dd_send, dd_recv, nm_send, nm_recv) = refs
    whole = {'up': wu, 'dn': wd}
    recv0 = {'up': r0u, 'dn': r0d}
    recvs = {'up': (q1u, q2u, q3u), 'dn': (q1d, q2d, q3d)}
    state_in = {'up': (acc_up, mas_up, mom_up, var_up), 'dn': (acc_dn, mas_dn, mom_dn, var_dn)}
    state_out = {'up': (None, o_mas_up, o_mom_up, o_var_up), 'dn': (None, o_mas_dn, o_mom_dn, o_var_dn)}
    w_out = {'up': o_wu, 'dn': o_wd}

    me = lax.axis_index('fsdp')
    bits = (me // 8, (me // 4) % 2, (me // 2) % 2)
    core = me % 2
    partner = me + 1 - 2 * core
    neighbours = tuple(me + step * (1 - 2 * bit) for bit, step in zip(bits, (8, 4, 2)))

    def local(src, dst, sem):
        return pltpu.make_async_copy(src, dst, sem)

    def remote(src, dst, send, recv, device):
        return pltpu.make_async_remote_copy(src_ref=src, dst_ref=dst, send_sem=send, recv_sem=recv, device_id=(device,), device_id_type=MESH)

    def st_block(kind, layer, k):
        if kind == 'up':
            return stu.at[layer, k]
        return std.at[span(4 * layer + k, DN_ROWS)]

    def state_loads(kind, layer):
        return [local(state_in[kind][k].at[layer], st_block(kind, layer, k), ld_sem.at[MATRIX[kind, layer], k]) for k in range(4)]

    def state_store(kind, layer, k):
        return local(st_block(kind, layer, k), state_out[kind][k].at[layer], out_sem.at[MATRIX[kind, layer], k])

    def w_store(kind):
        return local(whole[kind].at[1], w_out[kind], w_sem.at[MATRIX[kind, 0]])

    def first_loads(i):
        at = span(i, MT)
        return (local(x_all.at[1, 0, at], xa.at[at], first_sem.at[0, i]), local(dy_hbm.at[0, at], dy.at[at], first_sem.at[1, i]))

    x0_load = local(x_all.at[0, 0], xb, x_sem.at[2])
    xn_load = local(x_hbm.at[0], xa, x_sem.at[3])

    def tile_loads(t):
        layer, cols, slot = 1 - t // TILES, span(t % TILES, D), t % 2
        return (local(w_up.at[layer, :, cols], w1t.at[slot], wt_sem.at[0, slot]),
                local(w_dn.at[layer, cols], w2t.at[slot], wt_sem.at[1, slot]))

    def start(copies):
        for copy in copies:
            copy.start()

    def wait(copies):
        for copy in copies:
            copy.wait()

    start(first_loads(0) + tile_loads(0) + first_loads(1))

    barrier = pltpu.get_barrier_semaphore()

    def hello(k, carry):
        pl.semaphore_signal(barrier, inc=1, device_id=(lax.rem(me + k, NDEV),), device_id_type=MESH)
        return carry

    lax.fori_loop(1, NDEV, hello, 0)
    pl.semaphore_wait(barrier, NDEV - 1)

    def place(fixed):
        return tuple(fixed.get(d, ALL) for d in range(3))

    def chunk_cols(kind, k):
        return span(k, KINDS[kind][1] // KINDS[kind][3])

    def rs_core(kind, layer, k):
        m, cols = MATRIX[kind, layer], chunk_cols(kind, k)
        return remote(whole[kind].at[layer, :, :, :, 1 - core, :, cols], recv0[kind].at[:, :, :, :, cols], rs_send.at[m, k, 0], rs_recv.at[m, k, 0], partner)

    def rs_copies(kind, layer, stage, k):
        m, cols, third = MATRIX[kind, layer], chunk_cols(kind, k), KINDS[kind][0] // 3
        copies = []
        for p, dims in enumerate(DIM_ORDERS):
            fixed = {d: bits[d] for d in dims[:stage]}
            fixed[dims[stage]] = 1 - bits[dims[stage]]
            src = recv0[kind].at[place(fixed) + (pl.ds(third * p, third), cols)]
            dst = recvs[kind][stage].at[(p,) + (ALL,) * (3 - stage) + (cols,)]
            sem = 1 + 3 * stage + p
            copies.append(remote(src, dst, rs_send.at[m, k, sem], rs_recv.at[m, k, sem], neighbours[dims[stage]]))
        return copies

    def rs_begin(kind, layer, k=0):
        rs_core(kind, layer, k).start()

    def rs_first(kind, layer, k=0):
        rs_core(kind, layer, k).wait()
        cols = chunk_cols(kind, k)

        def add(i, carry):
            z, y, x = i // 4, (i // 2) % 2, i % 2
            recv0[kind][z, y, x, :, cols] = recv0[kind][z, y, x, :, cols] + whole[kind][layer, z, y, x, core, :, cols]
            return carry

        lax.fori_loop(0, 8, add, 0)
        start(rs_copies(kind, layer, 0, k))

    def rs_next(kind, layer, stage, k=0):
        cols, third = chunk_cols(kind, k), KINDS[kind][0] // 3
        buf, got = recv0[kind], recvs[kind][stage]
        arriving = rs_copies(kind, layer, stage, k)
        for p, dims in enumerate(DIM_ORDERS):
            arriving[p].wait()
            free = [d for d in range(3) if d in dims[stage + 1:]]
            for i in range(2 ** len(free)):
                where = {d: bits[d] for d in dims[:stage + 1]}
                slot = []
                for j, d in enumerate(free):
                    where[d] = (i >> (len(free) - 1 - j)) & 1
                    slot.append(where[d])
                idx = place(where) + (pl.ds(third * p, third), cols)
                buf[idx] = buf[idx] + got[(p,) + tuple(slot) + (ALL, cols)]
        start(rs_copies(kind, layer, stage + 1, k))

    def lamb(kind, layer):
        m = MATRIX[kind, layer]
        rows, cols, wide, chunks = KINDS[kind]
        third, per_row = rows // 3, cols // wide
        buf, got = recv0[kind], recvs[kind][2]
        st = functools.partial(st_block, kind, layer)
        wait(state_loads(kind, layer))
        for k in range(chunks):
            wait(rs_copies(kind, layer, 2, k))
        zero = jnp.zeros((2 * SUB, wide), F32)
        w_sum, u_sum = zero, zero
        for p in range(3):
            def chunk(i, carry):
                w_acc, u_acc = carry
                row, cs = i // per_row, span(i % per_row, wide)
                near = span(row, 2 * SUB)
                at = (pl.ds(pl.multiple_of(third * p + row * 2 * SUB, 2 * SUB), 2 * SUB), cs)
                total = buf[bits + at].astype(F32) + got[p, near, cs].astype(F32)
                master = st(1)[at]
                grad = (st(0)[at] + total) / MICRO_STEPS
                mom = BETA_MOM * st(2)[at] + (1.0 - BETA_MOM) * grad
                var = BETA_VAR * st(3)[at] + (1.0 - BETA_VAR) * grad * grad
                upd = (mom / (1.0 - BETA_MOM ** STEP_COUNT)) / (jnp.sqrt(var / (1.0 - BETA_VAR ** STEP_COUNT)) + ADAM_EPS) + WEIGHT_DECAY * master
                st(0)[at] = upd
                st(2)[at] = mom
                st(3)[at] = var
                return w_acc + master * master, u_acc + upd * upd

            w_sum, u_sum = lax.fori_loop(0, (third // (2 * SUB)) * per_row, chunk, (w_sum, u_sum))

        def fold(v):
            tiles = [v[SUB * i:SUB * i + SUB, LANES * j:LANES * j + LANES] for i in range(2) for j in range(wide // LANES)]
            return functools.reduce(lambda a, b: a + b, tiles)

        norms[m, me, 0:SUB] = fold(w_sum)
        norms[m, me, SUB:2 * SUB] = fold(u_sum)
        start([state_store(kind, layer, k) for k in (2, 3)])

        def tell(k, carry):
            remote(norms.at[m, me], norms.at[m, me], nm_send.at[m], nm_recv.at[m], lax.rem(me + k, NDEV)).start()
            return carry

        lax.fori_loop(1, NDEV, tell, 0)

    def apply(kind, layer):
        m = MATRIX[kind, layer]
        rows, cols, wide, _ = KINDS[kind]
        st = functools.partial(st_block, kind, layer)
        others = norms.at[m, pl.ds(0, NDEV - 1)]
        wait([local(others, others, sem.at[m]) for sem in (nm_send, nm_recv)])
        sums = jnp.sum(norms[m], axis=0)
        total = [jnp.sum(jnp.sum(v, axis=0, keepdims=True), axis=1, keepdims=True) for v in (sums[0:SUB], sums[SUB:2 * SUB])]
        scale = LEARN_RATE * (jnp.sqrt(total[0]) / jnp.sqrt(total[1]))
        per_row = cols // wide

        def chunk(i, carry):
            at = (span(i // per_row, 2 * SUB), span(i % per_row, wide))
            new = st(1)[at] - scale * st(0)[at]
            st(1)[at] = new
            whole[kind][(layer,) + bits + (core,) + at] = new.astype(BF16)
            return carry

        lax.fori_loop(0, (rows // (2 * SUB)) * per_row, chunk, 0)
        state_store(kind, layer, 1).start()

    def ag_copies(kind, layer, stage):
        m, third = MATRIX[kind, layer], KINDS[kind][0] // 3
        copies = []
        for p, dims in enumerate(DIM_ORDERS):
            ref = whole[kind].at[(layer,) + place({d: bits[d] for d in dims[:3 - stage]}) + (core, pl.ds(third * p, third))]
            copies.append(remote(ref, ref, ag_send.at[m, stage, p], ag_recv.at[m, stage, p], neighbours[dims[2 - stage]]))
        return copies

    def own_pass(kind, layer):
        m = MATRIX[kind, layer]
        ref = whole[kind].at[(layer,) + bits + (core,)]
        return remote(ref, ref, dd_send.at[m, 3, 0], dd_recv.at[m, 3, 0], partner)

    def pass_copies(kind, layer, stage):
        m, third = MATRIX[kind, layer], KINDS[kind][0] // 3
        copies = []
        for p, dims in enumerate(DIM_ORDERS):
            fixed = {d: bits[d] for d in dims[:2 - stage]}
            fixed[dims[2 - stage]] = 1 - bits[dims[2 - stage]]
            ref = whole[kind].at[(layer,) + place(fixed) + (core, pl.ds(third * p, third))]
            copies.append(remote(ref, ref, dd_send.at[m, stage, p], dd_recv.at[m, stage, p], partner))
        return copies

    def ag_begin(kind, layer):
        start(ag_copies(kind, layer, 0))
        own_pass(kind, layer).start()

    def ag_next(kind, layer, stage):
        wait(ag_copies(kind, layer, stage))
        if stage < 2:
            start(ag_copies(kind, layer, stage + 1))
        start(pass_copies(kind, layer, stage))

    def ag_end(kind, layer):
        own_pass(kind, layer).wait()
        for stage in range(3):
            wait(pass_copies(kind, layer, stage))
        if layer == 1:
            w_store(kind).start()

    def hidden(x_ref, slot, ready=None):
        def rows(i, carry):
            if ready is not None:
                ready(i)
            at = span(i, MT)
            pre = jnp.dot(x_ref[at, :], w1t[slot], preferred_element_type=F32)
            d_act = lax.dot_general(dy[at, :], w2t[slot], ROW_COL, preferred_element_type=F32)
            a, slope = gelu_parts(pre)
            ta[at, :] = a.astype(BF16)
            td[at, :] = (d_act * slope).astype(BF16)
            return carry

        lax.fori_loop(0, TOK // MT, rows, 0)

    def part_down(layer, f):
        def chunk(j, carry):
            out = lax.dot_general(ta[:, span(j, PAIR)], dy[...], COL_COL, preferred_element_type=F32)
            wd[layer, f // 2, f % 2, j] = out.astype(BF16).reshape(2, DN_ROWS, D)
            return carry

        lax.fori_loop(0, 2, chunk, 0)

    def part_up(layer, f, x_ref):
        def chunk(j, carry):
            out = lax.dot_general(x_ref[:, span(j, PAIR)], td[...], COL_COL, preferred_element_type=F32)
            wu[layer, j, :, :, :, :, span(f, D)] = out.astype(BF16).reshape(2, 2, 2, UP_ROWS, D)
            return carry

        lax.fori_loop(0, 2, chunk, 0)

    def back_input(slot):
        def rows(i, carry):
            at = span(i, MT)
            std[at, :] += lax.dot_general(td[at, :], w1t[slot], ROW_COL, preferred_element_type=F32)
            return carry

        lax.fori_loop(0, TOK // MT, rows, 0)

    def clear(i, carry):
        std[span(i, 64), :] = jnp.zeros((64, D), F32)
        return carry

    lax.fori_loop(0, TOK // 64, clear, 0)

    def upper(f, carry):
        slot = f % 2
        wait(tile_loads(f))

        def ready(i):
            @pl.when(f == 0)
            def _():
                wait(first_loads(i))

                @pl.when(i < 2)
                def _():
                    start(first_loads(i + 2))

        hidden(xa, slot, ready)
        start(tile_loads(f + 1))

        @pl.when(f == 1)
        def _():
            x0_load.start()
            start(state_loads('up', 1) + state_loads('up', 0))


        @pl.when(f > 0)
        def _():
            rs_next('up', 1, 0, f - 1)

        part_up(1, f, xa)
        rs_begin('up', 1, f)
        part_down(1, f)
        back_input(slot)
        rs_first('up', 1, f)

        @pl.when(f > 0)
        def _():
            rs_next('up', 1, 1, f - 1)

        return carry

    lax.fori_loop(0, TILES, upper, 0)
    rs_begin('dn', 1, 0)
    rs_begin('dn', 1, 1)
    xn_load.start()

    def next_dy(i, carry):
        at = span(i, 64)
        dy[at, :] = (dy[at, :].astype(F32) + std[at, :]).astype(BF16)
        return carry

    lax.fori_loop(0, TOK // 64, next_dy, 0)
    start(state_loads('dn', 1) + state_loads('dn', 0))
    x0_load.wait()

    last = TILES - 1
    after_hidden = (
        lambda: rs_next('up', 1, 0, last),
        lambda: rs_next('dn', 1, 1, 0),
        lambda: (rs_first('up', 0, 1), rs_next('dn', 1, 1, 1), ag_next('up', 1, 1)),
        lambda: (rs_first('up', 0, 2), lamb('dn', 1), rs_next('up', 0, 0, 0), rs_next('up', 0, 0, 1)),
    )
    after_down = (
        lambda: (rs_next('up', 1, 1, last), rs_first('dn', 1, 0), lamb('up', 1), rs_next('dn', 1, 0, 0), apply('up', 1)),
        lambda: (rs_next('dn', 1, 0, 1), ag_next('up', 1, 0), rs_first('up', 0, 0)),
        None,
        lambda: (rs_next('up', 0, 0, 2), apply('dn', 1), rs_begin('dn', 0, 0), rs_begin('dn', 0, 1), ag_begin('dn', 1)),
    )
    after_up = (
        lambda: (ag_begin('up', 1), rs_first('dn', 1, 1)),
    )

    def at_tile(f, steps):
        for k, step in enumerate(steps):
            if step is not None:
                @pl.when(f == k)
                def _(step=step):
                    step()

    def lower(f, carry):
        wait(tile_loads(TILES + f))

        @pl.when(f < TILES - 1)
        def _():
            start(tile_loads(TILES + 1 + f))

        hidden(xb, f % 2)
        at_tile(f, after_hidden)
        part_down(0, f)
        at_tile(f, after_down)
        part_up(0, f, xb)
        rs_begin('up', 0, f)
        at_tile(f, after_up)
        return carry

    lax.fori_loop(0, TILES, lower, 0)
    rs_next('up', 0, 1, 0)
    rs_next('up', 0, 1, 1)
    rs_next('up', 0, 1, 2)
    rs_first('dn', 0, 0)
    rs_first('up', 0, last)
    rs_first('dn', 0, 1)
    rs_next('up', 0, 0, last)
    rs_next('dn', 0, 0, 0)
    rs_next('up', 0, 1, last)
    rs_next('dn', 0, 0, 1)
    lamb('up', 0)
    rs_next('dn', 0, 1, 0)
    rs_next('dn', 0, 1, 1)
    apply('up', 0)
    ag_begin('up', 0)
    lamb('dn', 0)
    ag_next('up', 0, 0)
    apply('dn', 0)
    ag_begin('dn', 0)
    ag_next('up', 0, 1)
    ag_next('dn', 0, 0)
    ag_next('up', 0, 2)
    ag_next('dn', 0, 1)
    ag_end('up', 0)

    xn_load.wait()

    def up_part(base, act):
        def body(n, carry):
            w = wu[0, :, :, :, :, :, span(n, D)].reshape(D, D)
            pre = jnp.dot(xa[base:base + MT, :], w, preferred_element_type=F32)
            act[span(n, MT), :] = gelu_tanh(pre).astype(BF16)
            return carry

        lax.fori_loop(0, TILES, body, 0)

    def down_part(base, act):
        def body(i, carry):
            at = pl.ds(pl.multiple_of(base + i * 256, 256), 256)
            prod = None
            for n in range(TILES):
                w = wd[0, n // 2, n % 2].reshape(D, D)
                term = jnp.dot(act[pl.ds(pl.multiple_of(n * MT + i * 256, 256), 256), :], w, preferred_element_type=F32)
                prod = term if prod is None else prod + term
            xb[at, :] = (xa[at, :].astype(F32) + prod).astype(BF16)
            return carry

        lax.fori_loop(0, 2, body, 0)

    def x_store(half):
        rows = pl.ds(half * 2 * MT, 2 * MT)
        return local(xb.at[rows], o_x.at[rows], xo_sem.at[half])

    up_part(0, ta)
    ag_next('up', 1, 2)
    ag_next('dn', 1, 0)
    up_part(MT, td)
    ag_next('dn', 0, 2)
    ag_next('dn', 1, 1)
    ag_end('dn', 0)
    down_part(0, ta)
    down_part(MT, td)
    x_store(0).start()
    up_part(2 * MT, ta)
    ag_end('up', 1)
    up_part(3 * MT, td)
    ag_next('dn', 1, 2)
    down_part(2 * MT, ta)
    down_part(3 * MT, td)
    ag_end('dn', 1)
    x_store(1).start()
    wait([x_store(0), x_store(1), w_store('up'), w_store('dn')])
    for kind, layer in MATRIX:
        wait([state_store(kind, layer, k) for k in (1, 2, 3)])


def last_layer_kernel(x1, w_up, w_dn, *refs):
    ins, outs = refs[:6], refs[6:12]
    o_x, xv, xo, wu, wd, acc, s0, s1, s2, s3, s4, s5, x_sem, w_sem, in_sem, out_sem = refs[12:]
    held = (s0, s1, s2, s3, s4, s5)
    def x_load(i):
        return pltpu.make_async_copy(x1.at[span(i, MT)], xv.at[span(i, MT)], x_sem.at[i])

    ups = [pltpu.make_async_copy(w_up.at[:, pl.ds(n * D, D)], wu.at[:, pl.ds(n * D, D)], w_sem.at[n]) for n in range(TILES)]
    downs = [pltpu.make_async_copy(w_dn.at[pl.ds(n * D, D)], wd.at[pl.ds(n * D, D)], w_sem.at[4 + n]) for n in range(TILES)]
    gets = [pltpu.make_async_copy(i, h, in_sem.at[k]) for k, (i, h) in enumerate(zip(ins, held))]
    puts = [pltpu.make_async_copy(h, o, out_sem.at[k]) for k, (h, o) in enumerate(zip(held, outs))]
    x_load(0).start()
    ups[0].start()
    downs[0].start()
    x_load(1).start()

    def x_store(i):
        return pltpu.make_async_copy(xo.at[span(i, MT)], o_x.at[0, span(i, MT)], out_sem.at[6 + i])

    for n in range(TILES):
        ups[n].wait()
        downs[n].wait()
        if n < TILES - 1:
            ups[n + 1].start()
            downs[n + 1].start()

        def rows(i, carry):
            if n == 0:
                x_load(i).wait()

                @pl.when(i < 2)
                def _():
                    x_load(i + 2).start()

            at, tile = span(i, MT), slice(n * D, n * D + D)
            pre = jnp.dot(xv[at, :], wu[:, tile], preferred_element_type=F32)
            out = jnp.dot(gelu_tanh(pre).astype(BF16), wd[tile, :], preferred_element_type=F32)
            if n == 0:
                acc[at, :] = xv[at, :].astype(F32) + out
            elif n < TILES - 1:
                acc[at, :] += out
            else:
                xo[at, :] = (acc[at, :] + out).astype(BF16)
                x_store(i).start()
            return carry

        lax.fori_loop(0, TOK // MT, rows, 0)
        if n in (1, 2):
            for get, put in list(zip(gets, puts))[3 * n - 3:3 * n]:
                get.wait()
                put.start()
        if n < 2:
            for get in gets[3 * n:3 * n + 3]:
                get.start()
    for copy in puts + [x_store(i) for i in range(TOK // MT)]:
        copy.wait()


def whole_step(x_layers, dy_top, x_next, w_up, w_down, *states):
    cores = (2, 2, 2)
    sizes = [(r, c) for r, c, *_ in KINDS.values()]
    scratch = [pltpu.VMEM((2,) + cores + (2, r, c), BF16) for r, c in sizes]
    scratch += [pltpu.VMEM(cores + (r, c), BF16) for r, c in sizes]
    scratch += [pltpu.VMEM((3, 2, 2, r // 3, c), BF16) for r, c in sizes]
    scratch += [pltpu.VMEM((3, 2, r // 3, c), BF16) for r, c in sizes]
    scratch += [pltpu.VMEM((3, r // 3, c), BF16) for r, c in sizes]
    scratch += [pltpu.VMEM((2, 4, UP_ROWS, FF), F32), pltpu.VMEM((TOK, D), F32)]
    scratch += [pltpu.VMEM((TOK, D), BF16)] * 5
    scratch += [pltpu.VMEM((2, D, D), BF16)] * 2 + [pltpu.VMEM((4, NDEV, 16, 128), F32)]
    sem4 = (4, 4)
    rs_sem, ag_sem = DMA((4, TILES, 10)), DMA((4, 4, 3))
    scratch += [DMA(sem4), DMA((4,)), DMA((2, 4)), DMA(cores[1:]), DMA(sem4), DMA((2,)), DMA((2,)), rs_sem, rs_sem, ag_sem, ag_sem, ag_sem, ag_sem, DMA((4,)), DMA((4,))]
    state_shapes = [jax.ShapeDtypeStruct(s.shape, F32) for s in states[2:]]
    shapes = state_shapes + [jax.ShapeDtypeStruct((TOK, D), BF16)]
    shapes += [jax.ShapeDtypeStruct(cores + (2, r, c), BF16) for r, c in sizes]
    product = 2 * TOK * D * FF
    res = pl.pallas_call(
        step_kernel,
        out_shape=shapes,
        in_specs=[HBM] * 13,
        out_specs=[HBM] * 9,
        scratch_shapes=scratch,
        compiler_params=pltpu.CompilerParams(collective_id=0, has_side_effects=True, vmem_limit_bytes=67_000_000),
        cost_estimate=pl.CostEstimate(flops=11 * product, bytes_accessed=80_000_000, transcendentals=0),
        name='backward_update_gather',
    )(x_layers, dy_top, x_next, w_up, w_down, *states)
    x_mid, new_up, new_dn = res[6:]
    held = [pltpu.VMEM(s.shape, F32) for s in state_shapes]
    return pl.pallas_call(
        last_layer_kernel,
        out_shape=state_shapes + [jax.ShapeDtypeStruct(x_next.shape, BF16)],
        in_specs=[HBM] * 9,
        out_specs=[HBM] * 7,
        scratch_shapes=[pltpu.VMEM((TOK, D), BF16)] * 2 + [pltpu.VMEM((D, FF), BF16), pltpu.VMEM((FF, D), BF16), pltpu.VMEM((TOK, D), F32)] + held + [DMA((4,)), DMA((8,)), DMA((6,)), DMA((10,))],
        compiler_params=pltpu.CompilerParams(vmem_limit_bytes=60_000_000),
        cost_estimate=pl.CostEstimate(flops=2 * product, bytes_accessed=40_000_000, transcendentals=0),
        name='last_layer_forward',
    )(x_mid, new_up.reshape(D, FF), new_dn.reshape(FF, D), *res[:6])


def solution(mesh):
    shard_rows = P(None, 'fsdp')
    shard_batch = P('fsdp')
    spec_whole = P()

    def local_step(*args):
        return tuple(whole_step(*args))

    return jax.shard_map(local_step, mesh=mesh, in_specs=(shard_rows, shard_batch, shard_batch, spec_whole, spec_whole) + (shard_rows,) * 8, out_specs=(shard_rows,) * 6 + (shard_batch,), check_vma=False)
```
